32 devices in a mesh: cp: 8 (over y, x, core), tp: 4 (over z).
Axes of the slice: x: 2, y: 2, z: 4, core: 2. Of those that a mesh axis runs over, the one named last changes fastest.
Arguments:
- hidden: bfloat16 [2048, 4096], P('cp', 'tp'), may hold values from -120 to 120
- query_weight: bfloat16 [4096, 4096], P(None, 'tp'), may hold values from -0.1875 to 0.1875
- key_matrix: bfloat16 [4096, 512], P(None, 'tp'), may hold values from -0.09375 to 0.09375
- value_matrix: bfloat16 [4096, 512], P(None, 'tp'), may hold values from -0.09375 to 0.09375
- output_weight: bfloat16 [4096, 4096], P('tp'), may hold values from -0.1875 to 0.1875
- document_bounds: int32 [9], replicated, may hold values from 0 to 2048, as said below
- block_owner: int32 [16], replicated, may hold values from 0 to 7, as said below
Outputs:
- attended: bfloat16 [2048, 4096], P('cp', 'tp')
The draws below stay inside these ranges and needn't reach their ends.
Inputs may be any that keep to these rules, and one draw needn't show every extreme that they name: document_bounds[0] = 0, document_bounds[8] = 2048, strictly rising; document i holds the tokens from document_bounds[i] to document_bounds[i + 1] - 1. `block_owner`: every index of cp is named by exactly 2 blocks.
All inputs are finite; a program needn't handle non-finite values.
Results may differ from the reference program's by a relative error of at most 0.012.
The reference program's roundings to bfloat16 on the way (of `queries`, `values`, `heads_out` and `projected`) count: a program that leaves them out, or rounds other values in their place, can miss the bound.
Values may be sent and summed in bfloat16 or wider, within the bound.
A program may use at most 128 MiB of HBM per device.

```python
import math
import jax
import jax.numpy as jnp
from jax import lax

MODEL_WIDTH = 4096
QUERY_HEADS = 32
KEY_VALUE_HEADS = 4
HEAD_WIDTH = 128
BLOCK = 128
DOCS = 8
TOK_DEV = 256
PACKED_TOKENS = 2048
NBLK = 16


def draw_hidden(key, part):
    drawn = jax.random.normal(key, (PACKED_TOKENS, MODEL_WIDTH), jnp.float32)
    return jnp.clip(drawn, -6.0, 6.0).astype(jnp.bfloat16)


def draw_document_bounds(key, part):
    cut_points = jax.random.permutation(jax.random.fold_in(key, 21), PACKED_TOKENS - 1)[:DOCS - 1] + 1
    inner_cuts = jnp.sort(cut_points).astype(jnp.int32)
    return jnp.concatenate([jnp.zeros((1,), jnp.int32), inner_cuts, jnp.full((1,), PACKED_TOKENS, jnp.int32)])


def draw_block_owner(key, part):
    shuffled = jax.random.permutation(jax.random.fold_in(key, 31), NBLK)
    return (shuffled // (TOK_DEV // BLOCK)).astype(jnp.int32)


def steps_of(key, shape, pieces, low, largest):
    factor_of, own = 1.0, jax.random.fold_in(key, 6)
    for position, blocks in pieces:
        draws = jnp.exp(jax.random.uniform(jax.random.fold_in(own, position), (blocks,), jnp.float32, low / len(pieces), largest / len(pieces)))
        factor_of = factor_of * jnp.repeat(draws, shape[position] // blocks).reshape([-1 if axis == position else 1 for axis in range(len(shape))])
    return factor_of


def normal_values(own_key, shape, scale, most, shards=(), held_as=jnp.bfloat16):
    values = jax.random.normal(own_key, shape, jnp.float32) * scale
    if len(shards) > 0:
        values = steps_of(own_key, shape, shards, -0.22, 0.18) * values
    return jnp.clip(values, min=-most, max=most).astype(held_as)


def setup_inputs(seed: int = 0) -> dict:
    streams_of = jax.random.split(jax.random.key(seed), 8)
    return {
        "hidden": draw_hidden(jax.random.fold_in(streams_of[7], 71), 0),
        "query_weight": normal_values(streams_of[1], (MODEL_WIDTH, QUERY_HEADS * HEAD_WIDTH), (MODEL_WIDTH // 4) ** -0.5, 0.1875, ((1, 4),)),
        "key_matrix": normal_values(streams_of[2], (MODEL_WIDTH, KEY_VALUE_HEADS * HEAD_WIDTH), MODEL_WIDTH ** -0.5, 0.09375, ((1, 4),)),
        "value_matrix": normal_values(streams_of[3], (MODEL_WIDTH, KEY_VALUE_HEADS * HEAD_WIDTH), MODEL_WIDTH ** -0.5, 0.09375, ((1, 4),)),
        "output_weight": normal_values(streams_of[4], (QUERY_HEADS * HEAD_WIDTH, MODEL_WIDTH), (QUERY_HEADS * HEAD_WIDTH // 4) ** -0.5, 0.1875, ((0, 4),)),
        "document_bounds": draw_document_bounds(jax.random.fold_in(streams_of[7], 71), 0),
        "block_owner": draw_block_owner(jax.random.fold_in(streams_of[7], 71), 0),
    }


rope_theta = 500000.0
rope_factor = 8.0
rope_context = 8192.0
masked_score = -1e+30

def rope_inverse(head_size):
    halves = jnp.arange(head_size // 2, dtype=jnp.float32)
    inverse = 1.0 / rope_theta ** (2.0 * halves / head_size)
    wavelength = 2.0 * math.pi / inverse
    smooth = (rope_context / wavelength - 1.0) / 3.0
    blended = (1.0 - smooth) * inverse / rope_factor + smooth * inverse
    longer = jnp.where(wavelength > rope_context, inverse / rope_factor, blended)
    return jnp.where(wavelength < rope_context / 4.0, inverse, longer)

def document_of(tokens, bounds):
    inner_bounds = bounds[1:-1]
    return lax.optimization_barrier(jnp.sum((tokens[:, None] >= inner_bounds[None, :]).astype(jnp.int32), axis=1))

def position_of(tokens, bounds):
    starts = bounds[:-1]
    document_start = lax.optimization_barrier(jnp.max(jnp.where(starts[None, :] <= tokens[:, None], starts[None, :], 0), axis=1))
    return tokens - document_start

def rotate(raw_rows, tokens, bounds, head_size):
    row_count = raw_rows.shape[0]
    head_count = raw_rows.shape[1] // head_size
    angles = position_of(tokens, bounds).astype(jnp.float32)[:, None] * rope_inverse(head_size)[None, :]
    cosine = jnp.cos(angles)[:, None, :]
    sine_table = jnp.sin(angles)[:, None, :]
    heads_view = raw_rows.reshape(row_count, head_count, head_size)
    front_half = heads_view[:, :, :head_size // 2]
    back_half = heads_view[:, :, head_size // 2:]
    turned = jnp.concatenate([front_half * cosine - back_half * sine_table, back_half * cosine + front_half * sine_table], axis=2)
    return turned.reshape(row_count, head_count * head_size).astype(jnp.bfloat16)

def owner_order(block_owner, per_device):
    block_count = block_owner.shape[0]
    blocks = jnp.arange(block_count, dtype=jnp.int32)
    same_owner = block_owner[:, None] == block_owner[None, :]
    earlier = blocks[None, :] < blocks[:, None]
    owner_rank = lax.optimization_barrier(jnp.sum((same_owner & earlier).astype(jnp.int32), axis=1))
    target = block_owner * per_device + owner_rank
    return lax.optimization_barrier(jnp.sum(jnp.where(target[None, :] == blocks[:, None], blocks[None, :], 0), axis=1)).astype(jnp.int32)

def reference(hidden, query_weight, key_matrix, value_matrix, output_weight, document_bounds, block_owner):
    tokens = jnp.arange(PACKED_TOKENS, dtype=jnp.int32)
    query_raw = jnp.dot(hidden, query_weight, preferred_element_type=jnp.float32)
    key_raw = jnp.dot(hidden, key_matrix, preferred_element_type=jnp.float32)
    value_raw = jnp.dot(hidden, value_matrix, preferred_element_type=jnp.float32)
    queries = rotate(query_raw, tokens, document_bounds, HEAD_WIDTH)
    key_rows = rotate(key_raw, tokens, document_bounds, HEAD_WIDTH)
    value_rows = value_raw.astype(jnp.bfloat16)
    documents = document_of(tokens, document_bounds)
    query_heads = queries.reshape(PACKED_TOKENS, QUERY_HEADS, HEAD_WIDTH).transpose(1, 0, 2)
    per_head_keys = key_rows.reshape(PACKED_TOKENS, KEY_VALUE_HEADS, HEAD_WIDTH).transpose(1, 0, 2)
    per_head_values = value_rows.reshape(PACKED_TOKENS, KEY_VALUE_HEADS, HEAD_WIDTH).transpose(1, 0, 2)
    query_group_width = QUERY_HEADS // KEY_VALUE_HEADS
    query_block = math.gcd(PACKED_TOKENS, 1024)
    score_scale = 1.0 / math.sqrt(HEAD_WIDTH)

    def one_head(head_index):
        head_queries = query_heads[head_index]
        head_keys = per_head_keys[head_index // query_group_width]
        head_values = per_head_values[head_index // query_group_width]

        def one_block(block_index):
            first_row = block_index * query_block
            block_queries = lax.dynamic_slice_in_dim(head_queries, first_row, query_block, 0)
            block_tokens = first_row + jnp.arange(query_block, dtype=jnp.int32)
            block_documents = lax.dynamic_slice_in_dim(documents, first_row, query_block, 0)
            allowed = (block_documents[:, None] == documents[None, :]) & (tokens[None, :] <= block_tokens[:, None])
            scores = jnp.dot(block_queries, head_keys.T, preferred_element_type=jnp.float32) * score_scale
            scores = jnp.where(allowed, scores, masked_score)
            row_max = lax.optimization_barrier(jnp.max(scores, axis=1, keepdims=True))
            weights = jnp.where(allowed, jnp.exp(scores - row_max), 0.0)
            totals = lax.optimization_barrier(jnp.sum(weights, axis=1, keepdims=True))
            mixed_rows = jnp.dot(weights.astype(jnp.bfloat16), head_values, preferred_element_type=jnp.float32)
            return (mixed_rows / totals).astype(jnp.bfloat16)
        return lax.map(one_block, jnp.arange(PACKED_TOKENS // query_block, dtype=jnp.int32)).reshape(PACKED_TOKENS, HEAD_WIDTH)
    heads_out = lax.map(one_head, jnp.arange(QUERY_HEADS, dtype=jnp.int32))
    heads_out = heads_out.transpose(1, 0, 2).reshape(PACKED_TOKENS, QUERY_HEADS * HEAD_WIDTH)
    projected = jnp.dot(heads_out, output_weight, preferred_element_type=jnp.float32).astype(jnp.bfloat16)
    block_order = owner_order(block_owner, TOK_DEV // BLOCK)
    new_rows = (block_order[:, None] * BLOCK + jnp.arange(BLOCK, dtype=jnp.int32)[None, :]).reshape(-1)
    return jnp.take(projected, new_rows, axis=0)
```

```python
import functools
import math

import jax
import jax.numpy as jnp
from jax import lax
from jax.experimental import pallas as pl
from jax.experimental.pallas import tpu as pltpu
from jax.sharding import PartitionSpec as P

HEAD_WIDTH = 128
BLOCK = 128


rope_theta = 500000.0
rope_factor = 8.0
rope_context = 8192.0
masked_score = -1e30


def rope_inverse(head_size):
    halves = jnp.arange(head_size // 2, dtype=jnp.float32)
    inverse = 1.0 / rope_theta ** (2.0 * halves / head_size)
    wavelength = 2.0 * math.pi / inverse
    smooth = (rope_context / wavelength - 1.0) / 3.0
    blended = (1.0 - smooth) * inverse / rope_factor + smooth * inverse
    longer = jnp.where(wavelength > rope_context, inverse / rope_factor, blended)
    return jnp.where(wavelength < rope_context / 4.0, inverse, longer)


def document_of(tokens, bounds):
    inner_bounds = bounds[1:-1]
    return jnp.sum((tokens[:, None] >= inner_bounds[None, :]).astype(jnp.int32), axis=1)


def position_of(tokens, bounds):
    starts = bounds[:-1]
    document_start = jnp.max(
        jnp.where(starts[None, :] <= tokens[:, None], starts[None, :], 0), axis=1
    )
    return tokens - document_start


def rotate(raw_rows, tokens, bounds, head_size):
    row_count = raw_rows.shape[0]
    head_count = raw_rows.shape[1] // head_size
    angles = (
        position_of(tokens, bounds).astype(jnp.float32)[:, None] * rope_inverse(head_size)[None, :]
    )
    cosine = jnp.cos(angles)[:, None, :]
    sine_table = jnp.sin(angles)[:, None, :]
    heads_view = raw_rows.reshape(row_count, head_count, head_size)
    front_half = heads_view[:, :, : head_size // 2]
    back_half = heads_view[:, :, head_size // 2 :]
    turned = jnp.concatenate(
        [
            front_half * cosine - back_half * sine_table,
            back_half * cosine + front_half * sine_table,
        ],
        axis=2,
    )
    return turned.reshape(row_count, head_count * head_size).astype(jnp.bfloat16)


def owner_order(block_owner, per_device):
    block_count = block_owner.shape[0]
    blocks = jnp.arange(block_count, dtype=jnp.int32)
    same_owner = block_owner[:, None] == block_owner[None, :]
    earlier = blocks[None, :] < blocks[:, None]
    owner_rank = jnp.sum((same_owner & earlier).astype(jnp.int32), axis=1)
    target = block_owner * per_device + owner_rank
    return jnp.sum(jnp.where(target[None, :] == blocks[:, None], blocks[None, :], 0), axis=1)


def relayout(local_rows, block_order):
    cp_size = lax.axis_size("cp")
    row_count, row_width = local_rows.shape
    per_device = row_count // BLOCK
    portion = BLOCK // cp_size
    pieces = local_rows.reshape(per_device, cp_size, portion * row_width)
    spread = lax.all_to_all(pieces, "cp", split_axis=1, concat_axis=0, tiled=True)
    spread = spread.reshape(per_device * cp_size, portion * row_width)
    wanted = block_order.reshape(cp_size, per_device).T.reshape(-1)
    outgoing = jnp.take(spread, wanted, axis=0).reshape(per_device, cp_size, portion * row_width)
    arrived = lax.all_to_all(outgoing, "cp", split_axis=1, concat_axis=1, tiled=True)
    return arrived.reshape(row_count, row_width)


def project(local_rows, query_weight, key_matrix, value_matrix):
    weight_list = (query_weight, key_matrix, value_matrix)
    portion = lax.all_gather(local_rows, "tp", axis=1, tiled=True)
    return tuple(
        (jnp.dot(portion, weight, preferred_element_type=jnp.float32) for weight in weight_list)
    )


def attend(queries, query_tokens, key_rows, value_rows, key_tokens, bounds, head_size, kv_heads):
    row_count = queries.shape[0]
    query_group_width = queries.shape[1] // (kv_heads * head_size)
    grouped = queries.reshape(row_count, kv_heads, query_group_width, head_size).transpose(
        1, 2, 0, 3
    )
    grouped = grouped.reshape(kv_heads, query_group_width * row_count, head_size)
    query_documents = document_of(query_tokens, bounds)
    score_scale = 1.0 / math.sqrt(head_size)

    def update(flash_state, key_block, value_block, token_block):
        block_rows = key_block.shape[0]
        key_documents = document_of(token_block, bounds)
        allowed = (query_documents[:, None] == key_documents[None, :]) & (
            token_block[None, :] <= query_tokens[:, None]
        )
        running_max, running_sum, running_out = flash_state
        per_head_keys = key_block.reshape(block_rows, kv_heads, head_size).transpose(1, 0, 2)
        per_head_values = value_block.reshape(block_rows, kv_heads, head_size).transpose(1, 0, 2)
        scores = (
            jnp.einsum("khd,ksd->khs", grouped, per_head_keys, preferred_element_type=jnp.float32)
            * score_scale
        )
        wide_mask = jnp.tile(allowed, (query_group_width, 1))[None, :, :]
        scores = jnp.where(wide_mask, scores, masked_score)
        new_max = jnp.maximum(running_max, jnp.max(scores, axis=2))
        weights = jnp.where(wide_mask, jnp.exp(scores - new_max[:, :, None]), 0.0)
        factor = jnp.exp(running_max - new_max)
        new_sum = running_sum * factor + jnp.sum(weights, axis=2)
        new_out = running_out * factor[:, :, None] + jnp.einsum(
            "khs,ksd->khd",
            weights.astype(jnp.bfloat16),
            per_head_values,
            preferred_element_type=jnp.float32,
        )
        return (new_max, new_sum, new_out)

    initial = (
        jnp.full((kv_heads, query_group_width * row_count), masked_score, jnp.float32),
        jnp.zeros((kv_heads, query_group_width * row_count), jnp.float32),
        jnp.zeros((kv_heads, query_group_width * row_count, head_size), jnp.float32),
    )
    key_part = lax.all_gather(key_rows, "cp", axis=0, tiled=True)
    value_part = lax.all_gather(value_rows, "cp", axis=0, tiled=True)
    token_part = lax.all_gather(key_tokens, "cp", axis=0, tiled=True)
    part_rows = key_part.shape[0]
    block_rows = math.gcd(part_rows, 512)

    def one_block(block_index, inner_state):
        first_row = block_index * block_rows
        return update(
            inner_state,
            lax.dynamic_slice_in_dim(key_part, first_row, block_rows, 0),
            lax.dynamic_slice_in_dim(value_part, first_row, block_rows, 0),
            lax.dynamic_slice_in_dim(token_part, first_row, block_rows, 0),
        )

    final_max, final_sum, final_out = lax.fori_loop(0, part_rows // block_rows, one_block, initial)
    normalized = final_out / final_sum[:, :, None]
    merged = normalized.reshape(kv_heads, query_group_width, row_count, head_size).transpose(
        2, 0, 1, 3
    )
    return merged.reshape(row_count, kv_heads * query_group_width * head_size).astype(jnp.bfloat16)


def output_rows(heads_out, output_weight):
    head_terms = jnp.dot(heads_out, output_weight, preferred_element_type=jnp.float32)
    return lax.psum_scatter(head_terms.astype(jnp.bfloat16), "tp", scatter_dimension=1, tiled=True)


MESH = pl.DeviceIdType.MESH
VMEM_LIMIT = 62 << 20


def dot(a, b):
    return jnp.dot(a, b, preferred_element_type=jnp.float32)


def turn(raw, cosine, sine):
    half = raw.shape[1] // 2
    swapped = jnp.concatenate([raw[:, half:], raw[:, :half]], axis=1)
    return (raw * cosine + swapped * sine).astype(jnp.bfloat16)


def greet(n_cp, n_tp):
    c, z = lax.axis_index("cp"), lax.axis_index("tp")
    barrier = pltpu.get_barrier_semaphore()
    for t in range(1, n_cp):
        peer = lax.rem(c + t, n_cp)
        pl.semaphore_signal(barrier, inc=1, device_id={"cp": peer}, device_id_type=MESH)
    for t in range(1, n_tp):
        peer = lax.rem(z + t, n_tp)
        pl.semaphore_signal(barrier, inc=1, device_id={"tp": peer}, device_id_type=MESH)
    pl.semaphore_wait(barrier, n_cp + n_tp - 2)


def row_tokens(bounds, blocks, share, offset):
    shape = (blocks, share, HEAD_WIDTH)
    token = (
        lax.broadcasted_iota(jnp.int32, shape, 0) * BLOCK
        + lax.broadcasted_iota(jnp.int32, shape, 1) + offset
    )
    start = jnp.zeros_like(token)
    for i in range(bounds.shape[0] - 1):
        start = jnp.where(token >= bounds[i], bounds[i], start)
    return token, start


def fused_kernel(
    n_cp, n_tp,
    bounds, owner, hidden, wq_hbm, wk_hbm, wv_hbm, wo_hbm, inverse,
    out_ref,
    rows, w, wo, cosine, sine, tokens, starts, q_all, kv_own, kv_all,
    part, from_left, from_right, to_right, to_left, done, outgoing, landed, order,
    w_sem, o_sem, own_sem, s_send, s_recv, r_send, l_send, z_recv, k_send, k_recv,
    pr_send, pl_send, pr_recv, pl_recv, a_send, a_recv,
):
    c, z = lax.axis_index("cp"), lax.axis_index("tp")
    per, width = hidden.shape[0], hidden.shape[3]
    share = hidden.shape[2]
    count = per * share
    q_width = wq_hbm.shape[1]
    heads = q_width // HEAD_WIDTH
    end = n_tp - 1
    factor_of = math.log2(math.e) / math.sqrt(HEAD_WIDTH)
    weights = (
        pltpu.make_async_copy(wk_hbm, w.at[:, pl.ds(q_width, HEAD_WIDTH)], w_sem.at[1]),
        pltpu.make_async_copy(wv_hbm, w.at[:, pl.ds(q_width + HEAD_WIDTH, HEAD_WIDTH)], w_sem.at[2]),
        pltpu.make_async_copy(wq_hbm, w.at[:, pl.ds(0, q_width)], w_sem.at[0]),
    )

    def out_weight(o):
        return pltpu.make_async_copy(
            wo_hbm.at[:, pl.ds(o * width, width)], wo.at[o], o_sem.at[o]
        )

    own = pltpu.make_async_copy(hidden.at[:, c], rows.at[z, pl.ds(c * per, per)], own_sem)
    own.start()
    greet(n_cp, n_tp)

    def spread(i):
        peer = lax.rem(c + i, n_cp)
        return pltpu.make_async_remote_copy(
            src_ref=hidden.at[:, peer], dst_ref=rows.at[z, pl.ds(c * per, per)],
            send_sem=s_send.at[i], recv_sem=s_recv.at[i],
            device_id={"cp": peer}, device_id_type=MESH,
        )

    def along(origin, t, step):
        piece = rows.at[origin, pl.ds(t * per, per)]
        sems = r_send if step > 0 else l_send
        return pltpu.make_async_remote_copy(
            src_ref=piece, dst_ref=piece,
            send_sem=sems.at[origin, t], recv_sem=z_recv.at[origin, t],
            device_id={"tp": lax.rem(z + step + n_tp, n_tp)}, device_id_type=MESH,
        )

    def keys_to(i, t):
        span = pl.ds(t * per, per)
        return pltpu.make_async_remote_copy(
            src_ref=kv_own.at[span], dst_ref=kv_all.at[span, c],
            send_sem=k_send.at[i, t], recv_sem=k_recv.at[i, t],
            device_id={"cp": lax.rem(c + i, n_cp)}, device_id_type=MESH,
        )

    def rightward(o, t):
        return pltpu.make_async_remote_copy(
            src_ref=to_right.at[o, t], dst_ref=from_left.at[o, t],
            send_sem=pr_send.at[o, t], recv_sem=pr_recv.at[o, t],
            device_id={"tp": lax.rem(z + 1, n_tp)}, device_id_type=MESH,
        )

    def leftward(o, t):
        return pltpu.make_async_remote_copy(
            src_ref=to_left.at[o, t], dst_ref=from_right.at[o, t],
            send_sem=pl_send.at[o, t], recv_sem=pl_recv.at[o, t],
            device_id={"tp": lax.rem(z + n_tp - 1, n_tp)}, device_id_type=MESH,
        )

    def final(i):
        peer = lax.rem(c + i, n_cp)
        return pltpu.make_async_remote_copy(
            src_ref=outgoing.at[pl.ds(peer * per, per)], dst_ref=landed.at[:, c],
            send_sem=a_send.at[i], recv_sem=a_recv.at[i],
            device_id={"cp": peer}, device_id_type=MESH,
        )

    def outward(origin, t):
        @pl.when(z < end)
        def _():
            along(origin, t, 1).start()

        @pl.when(z > 0)
        def _():
            along(origin, t, -1).start()

    for i in range(1, n_cp):
        spread(i).start()
    for copy in weights:
        copy.start()
    for o in range(n_tp):
        out_weight(o).start()
    own.wait()
    outward(z, c)

    blocks = per * n_cp
    token, start = row_tokens(bounds, blocks, share, c * share)
    tokens[...] = token.reshape(-1, HEAD_WIDTH)
    starts[...] = start.reshape(-1, HEAD_WIDTH)
    angle = (token - start).astype(jnp.float32).reshape(-1, HEAD_WIDTH) * inverse[...]
    cosine[...] = jnp.cos(angle)
    lane = lax.broadcasted_iota(jnp.int32, angle.shape, 1)
    sine[...] = jnp.where(lane < HEAD_WIDTH // 2, -1.0, 1.0) * jnp.sin(angle)

    def gather(s):
        for d in range(n_tp):
            t = s + end - d

            @pl.when((t >= 0) & (t < n_cp))
            def _():
                if d == 0:
                    @pl.when(t != c)
                    def _():
                        spread(lax.rem(c - t + n_cp, n_cp)).wait_recv()
                        outward(z, t)
                else:
                    @pl.when(z - d >= 0)
                    def _():
                        along(z - d, t, 1).wait_recv()

                        @pl.when(z < end)
                        def _():
                            along(z - d, t, 1).start()

                    @pl.when(z + d < n_tp)
                    def _():
                        along(z + d, t, -1).wait_recv()

                        @pl.when(z > 0)
                        def _():
                            along(z + d, t, -1).start()

    def project(t):
        span = pl.ds(t * per, per)
        lines = pl.ds(pl.multiple_of(t * count, count), count)
        x = jnp.concatenate([rows[o, span].reshape(count, width) for o in range(n_tp)], axis=1)
        cos_t, sin_t = cosine[lines, :], sine[lines, :]
        raw = dot(x, w[:, q_width:])
        key = turn(raw[:, :HEAD_WIDTH], cos_t, sin_t)
        value = raw[:, HEAD_WIDTH:].astype(jnp.bfloat16)
        tile = jnp.concatenate([key, value], axis=1).reshape(per, share, 2 * HEAD_WIDTH)
        kv_own[span] = tile
        kv_all[span, pl.ds(c, 1)] = tile[:, None]
        for i in range(1, n_cp):
            keys_to(i, t).start()
        raw_q = dot(x, w[:, :q_width])
        for h in range(heads):
            q_all[t, h * count : (h + 1) * count] = turn(
                raw_q[:, h * HEAD_WIDTH : (h + 1) * HEAD_WIDTH], cos_t, sin_t
            )

    def attend(t):
        lines = pl.ds(pl.multiple_of(t * count, count), count)
        q = q_all[t]
        start = jnp.tile(starts[lines, :], (heads, 1))[:, :1]
        token = jnp.tile(tokens[lines, :], (heads, 1))[:, :1]
        keys = per * BLOCK

        def more(k, carry):
            top, total, out = carry
            u = t - k
            span = pl.ds(u * per, per)
            key = kv_all[span, :, :, :HEAD_WIDTH].reshape(keys, HEAD_WIDTH)
            value = kv_all[span, :, :, HEAD_WIDTH:].reshape(keys, HEAD_WIDTH)
            score = lax.dot_general(
                q, key, (((1,), (1,)), ((), ())), preferred_element_type=jnp.float32
            )
            index = u * keys + lax.broadcasted_iota(jnp.int32, score.shape, 1)
            score = jnp.where((index >= start) & (index <= token), score, masked_score)
            new_top = jnp.maximum(top, jnp.max(score, axis=1, keepdims=True))
            weight = jnp.exp2((score - new_top) * factor_of)
            factor = jnp.exp2((top - new_top) * factor_of)
            total = total * factor + jnp.sum(weight, axis=1, keepdims=True)
            out = out * factor + dot(weight.astype(jnp.bfloat16), value)
            return new_top, total, out

        lengths = (heads * count, 1)
        initial = (
            jnp.full(lengths, masked_score, jnp.float32),
            jnp.zeros(lengths, jnp.float32),
            jnp.zeros((heads * count, HEAD_WIDTH), jnp.float32),
        )
        _, total, out = lax.fori_loop(0, t + 1, more, initial)
        out = (out / total).astype(jnp.bfloat16)
        return jnp.concatenate([out[h * count : (h + 1) * count] for h in range(heads)], axis=1)

    def output(t, attended):
        high = z // (n_tp // 2)
        for k in range(n_tp):
            o = (1 - high) * (end - k) + high * k
            product = dot(attended, wo[o])
            go_right = (z == 0) & (o > z)
            go_left = (z == end) & (o < z)

            @pl.when(go_right)
            def _():
                to_right[o, t] = product.astype(jnp.bfloat16)
                rightward(o, t).start()

            @pl.when(go_left)
            def _():
                to_left[o, t] = product.astype(jnp.bfloat16)
                leftward(o, t).start()

            @pl.when(jnp.logical_not(go_right | go_left))
            def _():
                part[o, t] = product

    def reduce(s):
        t_right = s - 1 - z
        t_left = s - 1 - (end - z)

        @pl.when((z > 0) & (t_right >= 0) & (t_right < n_cp))
        def _():
            for o in range(end, 0, -1):
                @pl.when(o > z)
                def _():
                    rightward(o, t_right).wait_recv()
                    total = part[o, t_right] + from_left[o, t_right].astype(jnp.float32)
                    to_right[o, t_right] = total.astype(jnp.bfloat16)
                    rightward(o, t_right).start()

        @pl.when((z < end) & (t_left >= 0) & (t_left < n_cp))
        def _():
            for o in range(end):
                @pl.when(o < z)
                def _():
                    leftward(o, t_left).wait_recv()
                    total = part[o, t_left] + from_right[o, t_left].astype(jnp.float32)
                    to_left[o, t_left] = total.astype(jnp.bfloat16)
                    leftward(o, t_left).start()

    def finish(t):
        @pl.when(z > 0)
        def _():
            rightward(z, t).wait_recv()
            part[z, t] += from_left[z, t].astype(jnp.float32)

        @pl.when(z < end)
        def _():
            leftward(z, t).wait_recv()
            part[z, t] += from_right[z, t].astype(jnp.float32)

        done[pl.ds(t * per, per)] = part[z, t].astype(jnp.bfloat16).reshape(per, share, width)

    @pl.loop(0, n_cp + 2 * n_tp - 1)
    def _(step):
        s = step - end
        gather(s)
        reduce(s)

        @pl.when((s >= 0) & (s < n_cp))
        def _():
            @pl.when(s == 0)
            def _():
                for copy in weights:
                    copy.wait()

            project(s)

        @pl.when((s >= 1) & (s <= n_cp))
        def _():
            @pl.when(s == 1)
            def _():
                for o in range(n_tp):
                    out_weight(o).wait()

            for i in range(1, n_cp):
                keys_to(i, s - 1).wait_recv()
            output(s - 1, attend(s - 1))

        @pl.when(s >= n_tp)
        def _():
            finish(s - n_tp)

    for b in range(blocks):
        rank = jnp.int32(0)
        for e in range(b):
            rank += (owner[e] == owner[b]).astype(jnp.int32)
        order[b] = owner[b] * per + rank
    for b in range(blocks):
        def seek(e, found):
            return jnp.where(order[e] == b, e, found)
        source = lax.fori_loop(0, blocks, seek, jnp.int32(0))
        outgoing[b] = done[source]
    for i in range(1, n_cp):
        final(i).start()
    out_ref[:, pl.ds(c, 1)] = outgoing[pl.ds(c * per, per)][:, None]
    for i in range(1, n_cp):
        final(i).wait_recv()
        source = lax.rem(c - i + n_cp, n_cp)
        out_ref[:, pl.ds(source, 1)] = landed[:, pl.ds(source, 1)]
    for i in range(1, n_cp):
        spread(i).wait_send()
        final(i).wait_send()

    @pl.loop(0, n_cp)
    def _(t):
        for i in range(1, n_cp):
            keys_to(i, t).wait_send()
        for o in range(n_tp):
            @pl.when((z < end) & (o <= z))
            def _():
                along(o, t, 1).wait_send()

            @pl.when((z > 0) & (o >= z))
            def _():
                along(o, t, -1).wait_send()

            @pl.when(o > z)
            def _():
                rightward(o, t).wait_send()

            @pl.when(o < z)
            def _():
                leftward(o, t).wait_send()


def fused_call(bounds, owner, hidden, wq, wk, wv, wo, inverse, n_cp, n_tp):
    rows, width = hidden.shape
    per = rows // BLOCK
    share = BLOCK // n_cp
    blocks, count = per * n_cp, per * share
    heads = wq.shape[1] // HEAD_WIDTH
    pieces = hidden.reshape(per, n_cp, share, width)
    bf, f32, i32, dma = jnp.bfloat16, jnp.float32, jnp.int32, pltpu.SemaphoreType.DMA
    vmem = pl.BlockSpec(memory_space=pltpu.VMEM)
    hbm = pl.BlockSpec(memory_space=pltpu.HBM)
    smem = pl.BlockSpec(memory_space=pltpu.SMEM)
    slab = (n_tp, n_cp, count, width)
    kv_width = 2 * HEAD_WIDTH
    sems = dma((n_tp, n_cp))
    flops = 2 * rows * (wq.shape[0] * (wq.shape[1] + kv_width) + wo.shape[0] * wo.shape[1])
    out = pl.pallas_call(
        functools.partial(fused_kernel, n_cp, n_tp),
        out_shape=jax.ShapeDtypeStruct((per, n_cp, share, width), bf),
        in_specs=[smem, smem, hbm, hbm, hbm, hbm, hbm, vmem],
        out_specs=vmem,
        scratch_shapes=[
            pltpu.VMEM((n_tp, blocks, share, width), bf),
            pltpu.VMEM((wq.shape[0], wq.shape[1] + kv_width), bf),
            pltpu.VMEM((n_tp, wo.shape[0], width), bf),
            pltpu.VMEM((rows, HEAD_WIDTH), f32), pltpu.VMEM((rows, HEAD_WIDTH), f32),
            pltpu.VMEM((rows, HEAD_WIDTH), i32), pltpu.VMEM((rows, HEAD_WIDTH), i32),
            pltpu.VMEM((n_cp, heads * count, HEAD_WIDTH), bf),
            pltpu.VMEM((blocks, share, kv_width), bf),
            pltpu.VMEM((blocks, n_cp, share, kv_width), bf),
            pltpu.VMEM(slab, f32),
            pltpu.VMEM(slab, bf), pltpu.VMEM(slab, bf), pltpu.VMEM(slab, bf), pltpu.VMEM(slab, bf),
            pltpu.VMEM((blocks, share, width), bf),
            pltpu.VMEM((blocks, share, width), bf),
            pltpu.VMEM((per, n_cp, share, width), bf),
            pltpu.SMEM((blocks,), i32),
            dma((3,)), dma((n_tp,)), dma, dma((n_cp,)), dma((n_cp,)), sems, sems, sems,
            dma((n_cp, n_cp)), dma((n_cp, n_cp)),
            sems, sems, sems, sems, dma((n_cp,)), dma((n_cp,)),
        ],
        compiler_params=pltpu.CompilerParams(
            collective_id=1, has_side_effects=True, vmem_limit_bytes=VMEM_LIMIT
        ),
        cost_estimate=pl.CostEstimate(flops=flops, bytes_accessed=20 << 20, transcendentals=0),
    )(bounds, owner, pieces, wq, wk, wv, wo, inverse)
    return out.reshape(rows, width)


def local_fused(
    hidden, query_weight, key_matrix, value_matrix, output_weight, document_bounds, block_owner
):
    n_cp, n_tp = lax.axis_size("cp"), lax.axis_size("tp")
    inverse = jnp.tile(rope_inverse(HEAD_WIDTH), 2)[None, :]
    return fused_call(
        document_bounds, block_owner, hidden, query_weight, key_matrix, value_matrix,
        output_weight, inverse, n_cp, n_tp,
    )


def local_plain(
    hidden, query_weight, key_matrix, value_matrix, output_weight, document_bounds, block_owner
):
    cp_index = lax.axis_index("cp")
    row_count = hidden.shape[0]
    per_device = row_count // BLOCK
    block_order = owner_order(block_owner, per_device)
    own_blocks = lax.dynamic_slice_in_dim(block_order, cp_index * per_device, per_device, 0)
    new_tokens = (
        own_blocks[:, None] * BLOCK + jnp.arange(BLOCK, dtype=jnp.int32)[None, :]
    ).reshape(-1)
    kv_heads = key_matrix.shape[1] // HEAD_WIDTH
    moved = relayout(hidden, block_order)
    query_raw, key_raw, value_raw = project(moved, query_weight, key_matrix, value_matrix)
    queries = rotate(query_raw, new_tokens, document_bounds, HEAD_WIDTH)
    key_rows = rotate(key_raw, new_tokens, document_bounds, HEAD_WIDTH)
    value_rows = value_raw.astype(jnp.bfloat16)
    heads_out = attend(
        queries, new_tokens, key_rows, value_rows, new_tokens, document_bounds, HEAD_WIDTH, kv_heads
    )
    return output_rows(heads_out, output_weight)


def solution(mesh):
    shares = BLOCK // mesh.shape["cp"]
    local = local_fused if shares % 16 == 0 else local_plain
    placed = (P("cp", "tp"), P(None, "tp"), P(None, "tp"), P(None, "tp"), P("tp", None), P(), P())
    return jax.shard_map(
        local, mesh=mesh, in_specs=placed, out_specs=P("cp", "tp"), check_vma=False
    )
```

```python
import functools
import math

import jax
import jax.numpy as jnp
from jax import lax
from jax.experimental import pallas as pl
from jax.experimental.pallas import tpu as pltpu
from jax.sharding import PartitionSpec as P

HEAD_WIDTH = 128
BLOCK = 128


rope_theta = 500000.0
rope_factor = 8.0
rope_context = 8192.0
masked_score = -1e30


def rope_inverse(head_size):
    halves = jnp.arange(head_size // 2, dtype=jnp.float32)
    inverse = 1.0 / rope_theta ** (2.0 * halves / head_size)
    wavelength = 2.0 * math.pi / inverse
    smooth = (rope_context / wavelength - 1.0) / 3.0
    blended = (1.0 - smooth) * inverse / rope_factor + smooth * inverse
    longer = jnp.where(wavelength > rope_context, inverse / rope_factor, blended)
    return jnp.where(wavelength < rope_context / 4.0, inverse, longer)


def document_of(tokens, bounds):
    inner_bounds = bounds[1:-1]
    return jnp.sum((tokens[:, None] >= inner_bounds[None, :]).astype(jnp.int32), axis=1)


def position_of(tokens, bounds):
    starts = bounds[:-1]
    document_start = jnp.max(
        jnp.where(starts[None, :] <= tokens[:, None], starts[None, :], 0), axis=1
    )
    return tokens - document_start


def rotate(raw_rows, tokens, bounds, head_size):
    row_count = raw_rows.shape[0]
    head_count = raw_rows.shape[1] // head_size
    angles = (
        position_of(tokens, bounds).astype(jnp.float32)[:, None] * rope_inverse(head_size)[None, :]
    )
    cosine = jnp.cos(angles)[:, None, :]
    sine_table = jnp.sin(angles)[:, None, :]
    heads_view = raw_rows.reshape(row_count, head_count, head_size)
    front_half = heads_view[:, :, : head_size // 2]
    back_half = heads_view[:, :, head_size // 2 :]
    turned = jnp.concatenate(
        [
            front_half * cosine - back_half * sine_table,
            back_half * cosine + front_half * sine_table,
        ],
        axis=2,
    )
    return turned.reshape(row_count, head_count * head_size).astype(jnp.bfloat16)


def owner_order(block_owner, per_device):
    block_count = block_owner.shape[0]
    blocks = jnp.arange(block_count, dtype=jnp.int32)
    same_owner = block_owner[:, None] == block_owner[None, :]
    earlier = blocks[None, :] < blocks[:, None]
    owner_rank = jnp.sum((same_owner & earlier).astype(jnp.int32), axis=1)
    target = block_owner * per_device + owner_rank
    return jnp.sum(jnp.where(target[None, :] == blocks[:, None], blocks[None, :], 0), axis=1)


def relayout(local_rows, block_order):
    cp_size = lax.axis_size("cp")
    row_count, row_width = local_rows.shape
    per_device = row_count // BLOCK
    portion = BLOCK // cp_size
    pieces = local_rows.reshape(per_device, cp_size, portion * row_width)
    spread = lax.all_to_all(pieces, "cp", split_axis=1, concat_axis=0, tiled=True)
    spread = spread.reshape(per_device * cp_size, portion * row_width)
    wanted = block_order.reshape(cp_size, per_device).T.reshape(-1)
    outgoing = jnp.take(spread, wanted, axis=0).reshape(per_device, cp_size, portion * row_width)
    arrived = lax.all_to_all(outgoing, "cp", split_axis=1, concat_axis=1, tiled=True)
    return arrived.reshape(row_count, row_width)


def project(local_rows, query_weight, key_matrix, value_matrix):
    weight_list = (query_weight, key_matrix, value_matrix)
    portion = lax.all_gather(local_rows, "tp", axis=1, tiled=True)
    return tuple(
        (jnp.dot(portion, weight, preferred_element_type=jnp.float32) for weight in weight_list)
    )


def attend(queries, query_tokens, key_rows, value_rows, key_tokens, bounds, head_size, kv_heads):
    row_count = queries.shape[0]
    query_group_width = queries.shape[1] // (kv_heads * head_size)
    grouped = queries.reshape(row_count, kv_heads, query_group_width, head_size).transpose(
        1, 2, 0, 3
    )
    grouped = grouped.reshape(kv_heads, query_group_width * row_count, head_size)
    query_documents = document_of(query_tokens, bounds)
    score_scale = 1.0 / math.sqrt(head_size)

    def update(flash_state, key_block, value_block, token_block):
        block_rows = key_block.shape[0]
        key_documents = document_of(token_block, bounds)
        allowed = (query_documents[:, None] == key_documents[None, :]) & (
            token_block[None, :] <= query_tokens[:, None]
        )
        running_max, running_sum, running_out = flash_state
        per_head_keys = key_block.reshape(block_rows, kv_heads, head_size).transpose(1, 0, 2)
        per_head_values = value_block.reshape(block_rows, kv_heads, head_size).transpose(1, 0, 2)
        scores = (
            jnp.einsum("khd,ksd->khs", grouped, per_head_keys, preferred_element_type=jnp.float32)
            * score_scale
        )
        wide_mask = jnp.tile(allowed, (query_group_width, 1))[None, :, :]
        scores = jnp.where(wide_mask, scores, masked_score)
        new_max = jnp.maximum(running_max, jnp.max(scores, axis=2))
        weights = jnp.where(wide_mask, jnp.exp(scores - new_max[:, :, None]), 0.0)
        factor = jnp.exp(running_max - new_max)
        new_sum = running_sum * factor + jnp.sum(weights, axis=2)
        new_out = running_out * factor[:, :, None] + jnp.einsum(
            "khs,ksd->khd",
            weights.astype(jnp.bfloat16),
            per_head_values,
            preferred_element_type=jnp.float32,
        )
        return (new_max, new_sum, new_out)

    initial = (
        jnp.full((kv_heads, query_group_width * row_count), masked_score, jnp.float32),
        jnp.zeros((kv_heads, query_group_width * row_count), jnp.float32),
        jnp.zeros((kv_heads, query_group_width * row_count, head_size), jnp.float32),
    )
    key_part = lax.all_gather(key_rows, "cp", axis=0, tiled=True)
    value_part = lax.all_gather(value_rows, "cp", axis=0, tiled=True)
    token_part = lax.all_gather(key_tokens, "cp", axis=0, tiled=True)
    part_rows = key_part.shape[0]
    block_rows = math.gcd(part_rows, 512)

    def one_block(block_index, inner_state):
        first_row = block_index * block_rows
        return update(
            inner_state,
            lax.dynamic_slice_in_dim(key_part, first_row, block_rows, 0),
            lax.dynamic_slice_in_dim(value_part, first_row, block_rows, 0),
            lax.dynamic_slice_in_dim(token_part, first_row, block_rows, 0),
        )

    final_max, final_sum, final_out = lax.fori_loop(0, part_rows // block_rows, one_block, initial)
    normalized = final_out / final_sum[:, :, None]
    merged = normalized.reshape(kv_heads, query_group_width, row_count, head_size).transpose(
        2, 0, 1, 3
    )
    return merged.reshape(row_count, kv_heads * query_group_width * head_size).astype(jnp.bfloat16)


def output_rows(heads_out, output_weight):
    head_terms = jnp.dot(heads_out, output_weight, preferred_element_type=jnp.float32)
    return lax.psum_scatter(head_terms.astype(jnp.bfloat16), "tp", scatter_dimension=1, tiled=True)


MESH = pl.DeviceIdType.MESH
VMEM_LIMIT = 53 << 20


def dot(a, b):
    return jnp.dot(a, b, preferred_element_type=jnp.float32)


def turn(raw, cosine, sine):
    half = raw.shape[1] // 2
    swapped = jnp.concatenate([raw[:, half:], raw[:, :half]], axis=1)
    return (raw * cosine + swapped * sine).astype(jnp.bfloat16)


def greet(n_cp, n_tp):
    c, z = lax.axis_index("cp"), lax.axis_index("tp")
    barrier = pltpu.get_barrier_semaphore()
    for t in range(1, n_cp):
        peer = lax.rem(c + t, n_cp)
        pl.semaphore_signal(barrier, inc=1, device_id={"cp": peer}, device_id_type=MESH)
    for t in range(1, n_tp):
        peer = lax.rem(z + t, n_tp)
        pl.semaphore_signal(barrier, inc=1, device_id={"tp": peer}, device_id_type=MESH)
    pl.semaphore_wait(barrier, n_cp + n_tp - 2)


def row_tokens(bounds, blocks, share, offset):
    shape = (blocks, share, HEAD_WIDTH)
    token = (
        lax.broadcasted_iota(jnp.int32, shape, 0) * BLOCK
        + lax.broadcasted_iota(jnp.int32, shape, 1) + offset
    )
    start = jnp.zeros_like(token)
    for i in range(bounds.shape[0] - 1):
        start = jnp.where(token >= bounds[i], bounds[i], start)
    return token, start


def chunk_sizes(sources):
    if sources < 4 or sources % 2:
        return [1] * sources
    return [1] + [2] * ((sources - 2) // 2) + [1]


def fused_kernel(
    n_cp, n_tp, sizes,
    bounds, owner, hidden, wq_hbm, wk_hbm, wv_hbm, wo_hbm, inverse,
    out_ref,
    rows, w, wo, cosine, sine, tokens, starts, q_all, kv_own, kv_all,
    part, from_left, from_right, to_right, to_left, done, outgoing, landed, order,
    w_sem, o_sem, own_sem, s_send, s_recv, d_send, r_send, l_send, z_recv, k_send, k_recv,
    pr_send, pl_send, pr_recv, pl_recv, a_send, a_recv,
):
    c, z = lax.axis_index("cp"), lax.axis_index("tp")
    per, share, width = hidden.shape[0], hidden.shape[2], hidden.shape[3]
    blocks = per * n_cp
    unit = per * share
    q_width = wq_hbm.shape[1]
    heads = q_width // HEAD_WIDTH
    end = n_tp - 1
    last = len(sizes)
    firsts = [sum(sizes[:k]) for k in range(last + 1)]
    factor_of = math.log2(math.e) / math.sqrt(HEAD_WIDTH)
    weights = (
        pltpu.make_async_copy(wk_hbm, w.at[:, pl.ds(q_width, HEAD_WIDTH)], w_sem),
        pltpu.make_async_copy(wv_hbm, w.at[:, pl.ds(q_width + HEAD_WIDTH, HEAD_WIDTH)], w_sem),
        pltpu.make_async_copy(wq_hbm, w.at[:, pl.ds(0, q_width)], w_sem),
    )

    def out_weight(o):
        return pltpu.make_async_copy(
            wo_hbm.at[:, pl.ds(o * width, width)], wo.at[o], o_sem
        )

    own = pltpu.make_async_copy(hidden.at[:, c], rows.at[z, pl.ds(c * per, per)], own_sem)
    own.start()
    greet(n_cp, n_tp)

    def spread(i):
        peer = lax.rem(c + i, n_cp)
        return pltpu.make_async_remote_copy(
            src_ref=hidden.at[:, peer], dst_ref=rows.at[z, pl.ds(c * per, per)],
            send_sem=s_send, recv_sem=s_recv.at[i],
            device_id={"cp": peer}, device_id_type=MESH,
        )

    def along(origin, source, step):
        piece = rows.at[origin, pl.ds(source * per, per)]
        sems = r_send if step > 0 else l_send
        return pltpu.make_async_remote_copy(
            src_ref=piece, dst_ref=piece,
            send_sem=sems, recv_sem=z_recv.at[origin, source],
            device_id={"tp": lax.rem(z + step + n_tp, n_tp)}, device_id_type=MESH,
        )

    def skip(step):
        piece = rows.at[z, pl.ds(0, per)]
        return pltpu.make_async_remote_copy(
            src_ref=piece, dst_ref=piece,
            send_sem=d_send.at[(step + 1) // 2], recv_sem=z_recv.at[z, 0],
            device_id={"tp": lax.rem(z + 2 * step + n_tp, n_tp)}, device_id_type=MESH,
        )

    def blocks_of(k):
        return pl.ds(firsts[k] * per, sizes[k] * per)

    def lines_of(k):
        return pl.ds(firsts[k] * unit, sizes[k] * unit)

    def keys_to(i, k):
        return pltpu.make_async_remote_copy(
            src_ref=kv_own.at[blocks_of(k)], dst_ref=kv_all.at[blocks_of(k), c],
            send_sem=k_send, recv_sem=k_recv.at[k],
            device_id={"cp": lax.rem(c + i, n_cp)}, device_id_type=MESH,
        )

    def rightward(o, k):
        return pltpu.make_async_remote_copy(
            src_ref=to_right.at[o, lines_of(k)], dst_ref=from_left.at[o, lines_of(k)],
            send_sem=pr_send, recv_sem=pr_recv.at[o - 1, k],
            device_id={"tp": lax.rem(z + 1, n_tp)}, device_id_type=MESH,
        )

    def leftward(o, k):
        return pltpu.make_async_remote_copy(
            src_ref=to_left.at[o, lines_of(k)], dst_ref=from_right.at[o, lines_of(k)],
            send_sem=pl_send, recv_sem=pl_recv.at[o, k],
            device_id={"tp": lax.rem(z + n_tp - 1, n_tp)}, device_id_type=MESH,
        )

    def final(i):
        peer = lax.rem(c + i, n_cp)
        return pltpu.make_async_remote_copy(
            src_ref=outgoing.at[pl.ds(peer * per, per)], dst_ref=landed.at[:, c],
            send_sem=a_send, recv_sem=a_recv,
            device_id={"cp": peer}, device_id_type=MESH,
        )

    for i in range(1, n_cp):
        spread(i).start()
    for copy in weights:
        copy.start()
    for o in range(n_tp):
        out_weight(o).start()

    token, start = row_tokens(bounds, blocks, share, c * share)
    tokens[...] = token.reshape(-1, HEAD_WIDTH)
    starts[...] = start.reshape(-1, HEAD_WIDTH)
    angle = (token - start).astype(jnp.float32).reshape(-1, HEAD_WIDTH) * inverse[...]
    cosine[...] = jnp.cos(angle)
    lane = lax.broadcasted_iota(jnp.int32, angle.shape, 1)
    sine[...] = jnp.where(lane < HEAD_WIDTH // 2, -1.0, 1.0) * jnp.sin(angle)
    slots = []
    for b in range(blocks):
        rank = jnp.int32(0)
        for e in range(b):
            rank += (owner[e] == owner[b]).astype(jnp.int32)
        slots.append(owner[b] * per + rank)
    for b in range(blocks):
        found = jnp.int32(0)
        for e in range(1, blocks):
            found = jnp.where(slots[e] == b, e, found)
        order[b] = found
    own.wait()

    inner = (z > 0) & (z < end)

    def take(source):
        @pl.when(source != c)
        def _():
            spread(lax.rem(c - source + n_cp, n_cp)).wait_recv()

    def end_sends(source):
        @pl.when(z == 0)
        def _():
            along(z, source, 1).start()

        @pl.when(z == end)
        def _():
            along(z, source, -1).start()

    def first_sends():
        for step in (1, -1):
            @pl.when((z + step >= 0) & (z + step < n_tp))
            def _():
                along(z, 0, step).start()

            @pl.when((z + 2 * step >= 0) & (z + 2 * step < n_tp))
            def _():
                skip(step).start()

    def first_waits():
        for d in range(1, n_tp):
            for step in (1, -1):
                @pl.when((z - step * d >= 0) & (z - step * d < n_tp))
                def _():
                    along(z - step * d, 0, step).wait_recv()
                    if d > 1:
                        @pl.when((z + step >= 0) & (z + step < n_tp))
                        def _():
                            along(z - step * d, 0, step).start()

    def end_waits(source):
        for d in range(1, n_tp):
            @pl.when(z == end)
            def _():
                along(z - d, source, 1).wait_recv()

            @pl.when(z == 0)
            def _():
                along(z + d, source, -1).wait_recv()

    def flow(source, d, near):
        if source >= n_cp:
            return
        rights = (z == end - 1) if near else (z < end - 1)
        lefts = (z == 1) if near else (z > 1)

        @pl.when(inner & rights & (z - d >= 0))
        def _():
            if d > 0:
                along(z - d, source, 1).wait_recv()
            along(z - d, source, 1).start()

        @pl.when(inner & lefts & (z + d < n_tp))
        def _():
            if d > 0:
                along(z + d, source, -1).wait_recv()
            along(z + d, source, -1).start()

    def far(source):
        with jax.named_scope("far"):
            for d in range(1, end):
                flow(source, d, False)
            flow(source + 2, 0, False)

    def near(source):
        with jax.named_scope("near"):
            for d in range(1, end):
                flow(source, d, True)
            flow(source + 2, 0, True)

    def ends(source):
        with jax.named_scope("ends"):
            end_waits(source)

    def project(k):
        count = sizes[k] * unit
        x = jnp.concatenate(
            [rows[o, blocks_of(k)].reshape(count, width) for o in range(n_tp)], axis=1
        )
        cos_t, sin_t = cosine[lines_of(k), :], sine[lines_of(k), :]
        raw = dot(x, w[:, q_width:])
        key = turn(raw[:, :HEAD_WIDTH], cos_t, sin_t)
        value = raw[:, HEAD_WIDTH:].astype(jnp.bfloat16)
        tile = jnp.concatenate([key, value], axis=1)
        tile = tile.reshape(sizes[k] * per, share, 2 * HEAD_WIDTH)
        kv_own[blocks_of(k)] = tile
        kv_all[blocks_of(k), pl.ds(c, 1)] = tile[:, None]
        for i in range(1, n_cp):
            keys_to(i, k).start()
        raw_q = dot(x, w[:, :q_width])
        for h in range(heads):
            q_all[pl.ds(firsts[k] * unit * heads + h * count, count), :] = turn(
                raw_q[:, h * HEAD_WIDTH : (h + 1) * HEAD_WIDTH], cos_t, sin_t
            )

    def attend(k):
        count = sizes[k] * unit
        q = q_all[pl.ds(firsts[k] * unit * heads, heads * count), :]
        start = jnp.tile(starts[lines_of(k), :], (heads, 1))[:, :1]
        token = jnp.tile(tokens[lines_of(k), :], (heads, 1))[:, :1]

        def scored(source, size, diagonal):
            keys = size * per * BLOCK
            span = pl.ds(source * per, size * per)
            key = kv_all[span, :, :, :HEAD_WIDTH].reshape(keys, HEAD_WIDTH)
            value = kv_all[span, :, :, HEAD_WIDTH:].reshape(keys, HEAD_WIDTH)
            score = lax.dot_general(
                q, key, (((1,), (1,)), ((), ())), preferred_element_type=jnp.float32
            )
            index = source * (per * BLOCK) + lax.broadcasted_iota(jnp.int32, score.shape, 1)
            allowed = index >= start
            if diagonal:
                allowed = allowed & (index <= token)
            return jnp.where(allowed, score, masked_score), value

        def lane_sums(weight):
            partial = weight[:, :HEAD_WIDTH]
            for g in range(1, weight.shape[1] // HEAD_WIDTH):
                partial = partial + weight[:, g * HEAD_WIDTH : (g + 1) * HEAD_WIDTH]
            return partial

        def more(source, size, diagonal, carry):
            top, total, out = carry
            score, value = scored(source, size, diagonal)
            new_top = jnp.maximum(top, jnp.max(score, axis=1, keepdims=True))
            weight = jnp.exp2((score - new_top) * factor_of)
            factor = jnp.exp2((top - new_top) * factor_of)
            total = total * factor + lane_sums(weight)
            out = out * factor + dot(weight.astype(jnp.bfloat16), value)
            return new_top, total, out

        lengths = (heads * count, 1)
        carry = (
            jnp.full(lengths, masked_score, jnp.float32),
            jnp.zeros((heads * count, HEAD_WIDTH), jnp.float32),
            jnp.zeros((heads * count, HEAD_WIDTH), jnp.float32),
        )
        pairs = firsts[k] // 2
        if pairs > 0:
            carry = lax.fori_loop(0, pairs, lambda j, held: more(2 * j, 2, False, held), carry)
        if firsts[k] % 2:
            carry = more(firsts[k] - 1, 1, False, carry)
        with jax.named_scope("kvwait"):
            arrive(k)
        carry = more(firsts[k], sizes[k], True, carry)
        _, total, out = carry
        out = (out / jnp.sum(total, axis=1, keepdims=True)).astype(jnp.bfloat16)
        return jnp.concatenate([out[h * count : (h + 1) * count] for h in range(heads)], axis=1)

    def output(k, attended):
        high = z // (n_tp // 2)
        for turn_of in range(n_tp):
            o = (1 - high) * (end - turn_of) + high * turn_of
            product = dot(attended, wo[o])
            go_right = (z == 0) & (o > z)
            go_left = (z == end) & (o < z)

            @pl.when(go_right)
            def _():
                to_right[o, lines_of(k)] = product.astype(jnp.bfloat16)
                rightward(o, k).start()

            @pl.when(go_left)
            def _():
                to_left[o, lines_of(k)] = product.astype(jnp.bfloat16)
                leftward(o, k).start()

            @pl.when(jnp.logical_not(go_right | go_left))
            def _():
                part[o, lines_of(k)] = product

    def hop(k, h):
        lines = lines_of(k)

        @pl.when(z == h)
        def _():
            for o in range(end, h, -1):
                rightward(o, k).wait_recv()
                total = part[o, lines] + from_left[o, lines].astype(jnp.float32)
                to_right[o, lines] = total.astype(jnp.bfloat16)
                rightward(o, k).start()

        @pl.when(z == end - h)
        def _():
            for o in range(end - h):
                leftward(o, k).wait_recv()
                total = part[o, lines] + from_right[o, lines].astype(jnp.float32)
                to_left[o, lines] = total.astype(jnp.bfloat16)
                leftward(o, k).start()

    def finish(k):
        lines = lines_of(k)

        @pl.when(z > 0)
        def _():
            rightward(z, k).wait_recv()
            part[z, lines] += from_left[z, lines].astype(jnp.float32)

        @pl.when(z < end)
        def _():
            leftward(z, k).wait_recv()
            part[z, lines] += from_right[z, lines].astype(jnp.float32)

        summed = part[z, lines].astype(jnp.bfloat16)
        done[blocks_of(k)] = summed.reshape(sizes[k] * per, share, width)

    def arrive(k):
        landed_keys = kv_all.at[blocks_of(k), pl.ds(0, n_cp - 1)]
        pltpu.make_async_copy(landed_keys, landed_keys, k_recv.at[k]).wait()

    def reduce(k, h):
        with jax.named_scope("reduce"):
            hop(k, h)

    with jax.named_scope("fill"):
        for source in range(n_cp):
            take(source)
            if source == 0:
                first_sends()
                continue
            end_sends(source)
            if source <= 2:
                flow(source, 0, False)
                flow(source, 0, True)
        first_waits()
    pltpu.make_async_copy(w, w, w_sem).wait()
    passed, reached = 0, 0

    def pass_on(fars, nears):
        nonlocal passed, reached
        while passed < min(fars, n_cp - 1):
            passed += 1
            far(passed)
        while reached < min(nears, n_cp - 1):
            reached += 1
            near(reached)

    for k in range(last):
        pass_on(2 * firsts[k] + 2 * sizes[k] - 2, firsts[k + 1] - 1)
        for source in range(max(firsts[k], 1), firsts[k + 1]):
            ends(source)
        with jax.named_scope("project"):
            project(k)
        if k == 0:
            pass_on(2, 0)
            pltpu.make_async_copy(wo, wo, o_sem).wait()
        else:
            pass_on(n_cp if k > 1 else 5, firsts[k + 1])
        if k == last - 1:
            for e in range(last - 2):
                reduce(e, end - 1)
        with jax.named_scope("attend"):
            attended = attend(k)
        pass_on(n_cp if k > 0 else 3, firsts[k + 1] + (1 if k > 0 else 0))
        with jax.named_scope("output"):
            output(k, attended)
        if k > 0 and k < last - 1:
            for h in range(1, end - 1):
                if k - h >= 0:
                    reduce(k - h, h)
    with jax.named_scope("finish"):
        for k in range(last - 2):
            finish(k)
    for k in range(max(last - 2, 0), last):
        for h in range(1, end):
            reduce(k, h)
    with jax.named_scope("finish"):
        for k in range(max(last - 2, 0), last):
            finish(k)

    with jax.named_scope("a2a"):
        for b in range(blocks):
            outgoing[b] = done[order[b]]
        for i in range(1, n_cp):
            final(i).start()
        out_ref[:, pl.ds(c, 1)] = outgoing[pl.ds(c * per, per)][:, None]
        others = landed.at[:, pl.ds(0, n_cp - 1)]
        pltpu.make_async_copy(others, others, a_recv).wait()
        for i in range(1, n_cp):
            source = lax.rem(c - i + n_cp, n_cp)
            out_ref[:, pl.ds(source, 1)] = landed[:, pl.ds(source, 1)]

    def drain(ref, sem):
        pltpu.make_async_copy(ref, ref, sem).wait()

    drain(landed.at[:, pl.ds(0, n_cp - 1)], s_send)
    drain(landed.at[:, pl.ds(0, n_cp - 1)], a_send)
    drain(kv_all.at[:, pl.ds(0, n_cp - 1)], k_send)
    for step in (1, -1):
        @pl.when((z + 2 * step >= 0) & (z + 2 * step < n_tp))
        def _():
            skip(step).wait_send()

    for v in range(n_tp):
        @pl.when(z == v)
        def _():
            if v < end:
                pieces = (n_cp - 1) * (v + 1) + max(v, 1)
                drain(wo.at[0, pl.ds(0, pieces * unit)], r_send)
                drain(to_right.at[pl.ds(0, end - v)], pr_send)
            if v > 0:
                pieces = (n_cp - 1) * (n_tp - v) + max(end - v, 1)
                drain(wo.at[0, pl.ds(0, pieces * unit)], l_send)
                drain(to_left.at[pl.ds(0, v)], pl_send)


def fused_call(bounds, owner, hidden, wq, wk, wv, wo, inverse, n_cp, n_tp):
    rows, width = hidden.shape
    per = rows // BLOCK
    share = BLOCK // n_cp
    blocks = per * n_cp
    heads = wq.shape[1] // HEAD_WIDTH
    sizes = chunk_sizes(n_cp)
    pieces = hidden.reshape(per, n_cp, share, width)
    bf, f32, i32, dma = jnp.bfloat16, jnp.float32, jnp.int32, pltpu.SemaphoreType.DMA
    vmem = pl.BlockSpec(memory_space=pltpu.VMEM)
    hbm = pl.BlockSpec(memory_space=pltpu.HBM)
    smem = pl.BlockSpec(memory_space=pltpu.SMEM)
    slab = (n_tp, rows, width)
    kv_width = 2 * HEAD_WIDTH
    sums = dma((n_tp - 1, len(sizes)))
    flops = 2 * rows * (wq.shape[0] * (wq.shape[1] + kv_width) + wo.shape[0] * wo.shape[1])
    out = pl.pallas_call(
        functools.partial(fused_kernel, n_cp, n_tp, sizes),
        out_shape=jax.ShapeDtypeStruct((per, n_cp, share, width), bf),
        in_specs=[smem, smem, hbm, hbm, hbm, hbm, hbm, vmem],
        out_specs=vmem,
        scratch_shapes=[
            pltpu.VMEM((n_tp, blocks, share, width), bf),
            pltpu.VMEM((wq.shape[0], wq.shape[1] + kv_width), bf),
            pltpu.VMEM((n_tp, wo.shape[0], width), bf),
            pltpu.VMEM((rows, HEAD_WIDTH), f32), pltpu.VMEM((rows, HEAD_WIDTH), f32),
            pltpu.VMEM((rows, HEAD_WIDTH), i32), pltpu.VMEM((rows, HEAD_WIDTH), i32),
            pltpu.VMEM((rows * heads, HEAD_WIDTH), bf),
            pltpu.VMEM((blocks, share, kv_width), bf),
            pltpu.VMEM((blocks, n_cp, share, kv_width), bf),
            pltpu.VMEM(slab, f32),
            pltpu.VMEM(slab, bf), pltpu.VMEM(slab, bf), pltpu.VMEM(slab, bf), pltpu.VMEM(slab, bf),
            pltpu.VMEM((blocks, share, width), bf),
            pltpu.VMEM((blocks, share, width), bf),
            pltpu.VMEM((per, n_cp, share, width), bf),
            pltpu.SMEM((blocks,), i32),
            dma, dma, dma, dma, dma((n_cp,)), dma((2,)), dma, dma, dma((n_tp, n_cp)),
            dma, dma((len(sizes),)), dma, dma, sums, sums, dma, dma,
        ],
        compiler_params=pltpu.CompilerParams(
            collective_id=1, has_side_effects=True, vmem_limit_bytes=VMEM_LIMIT
        ),
        cost_estimate=pl.CostEstimate(flops=flops, bytes_accessed=20 << 20, transcendentals=0),
    )(bounds, owner, pieces, wq, wk, wv, wo, inverse)
    return out.reshape(rows, width)


def local_fused(
    hidden, query_weight, key_matrix, value_matrix, output_weight, document_bounds, block_owner
):
    n_cp, n_tp = lax.axis_size("cp"), lax.axis_size("tp")
    inverse = jnp.tile(rope_inverse(HEAD_WIDTH), 2)[None, :]
    return fused_call(
        document_bounds, block_owner, hidden, query_weight, key_matrix, value_matrix,
        output_weight, inverse, n_cp, n_tp,
    )


def local_plain(
    hidden, query_weight, key_matrix, value_matrix, output_weight, document_bounds, block_owner
):
    cp_index = lax.axis_index("cp")
    row_count = hidden.shape[0]
    per_device = row_count // BLOCK
    block_order = owner_order(block_owner, per_device)
    own_blocks = lax.dynamic_slice_in_dim(block_order, cp_index * per_device, per_device, 0)
    new_tokens = (
        own_blocks[:, None] * BLOCK + jnp.arange(BLOCK, dtype=jnp.int32)[None, :]
    ).reshape(-1)
    kv_heads = key_matrix.shape[1] // HEAD_WIDTH
    moved = relayout(hidden, block_order)
    query_raw, key_raw, value_raw = project(moved, query_weight, key_matrix, value_matrix)
    queries = rotate(query_raw, new_tokens, document_bounds, HEAD_WIDTH)
    key_rows = rotate(key_raw, new_tokens, document_bounds, HEAD_WIDTH)
    value_rows = value_raw.astype(jnp.bfloat16)
    heads_out = attend(
        queries, new_tokens, key_rows, value_rows, new_tokens, document_bounds, HEAD_WIDTH, kv_heads
    )
    return output_rows(heads_out, output_weight)


def solution(mesh):
    shares = BLOCK // mesh.shape["cp"]
    local = local_fused if shares % 16 == 0 else local_plain
    placed = (P("cp", "tp"), P(None, "tp"), P(None, "tp"), P(None, "tp"), P("tp", None), P(), P())
    return jax.shard_map(
        local, mesh=mesh, in_specs=placed, out_specs=P("cp", "tp"), check_vma=False
    )
```

```python
import functools
import math

import jax
import jax.numpy as jnp
from jax import lax
from jax.experimental import pallas as pl
from jax.experimental.pallas import tpu as pltpu
from jax.sharding import PartitionSpec as P

HEAD_WIDTH = 128
BLOCK = 128


rope_theta = 500000.0
rope_factor = 8.0
rope_context = 8192.0
masked_score = -1e30


def rope_inverse(head_size):
    halves = jnp.arange(head_size // 2, dtype=jnp.float32)
    inverse = 1.0 / rope_theta ** (2.0 * halves / head_size)
    wavelength = 2.0 * math.pi / inverse
    smooth = (rope_context / wavelength - 1.0) / 3.0
    blended = (1.0 - smooth) * inverse / rope_factor + smooth * inverse
    longer = jnp.where(wavelength > rope_context, inverse / rope_factor, blended)
    return jnp.where(wavelength < rope_context / 4.0, inverse, longer)


def document_of(tokens, bounds):
    inner_bounds = bounds[1:-1]
    return jnp.sum((tokens[:, None] >= inner_bounds[None, :]).astype(jnp.int32), axis=1)


def position_of(tokens, bounds):
    starts = bounds[:-1]
    document_start = jnp.max(
        jnp.where(starts[None, :] <= tokens[:, None], starts[None, :], 0), axis=1
    )
    return tokens - document_start


def rotate(raw_rows, tokens, bounds, head_size):
    row_count = raw_rows.shape[0]
    head_count = raw_rows.shape[1] // head_size
    angles = (
        position_of(tokens, bounds).astype(jnp.float32)[:, None] * rope_inverse(head_size)[None, :]
    )
    cosine = jnp.cos(angles)[:, None, :]
    sine_table = jnp.sin(angles)[:, None, :]
    heads_view = raw_rows.reshape(row_count, head_count, head_size)
    front_half = heads_view[:, :, : head_size // 2]
    back_half = heads_view[:, :, head_size // 2 :]
    turned = jnp.concatenate(
        [
            front_half * cosine - back_half * sine_table,
            back_half * cosine + front_half * sine_table,
        ],
        axis=2,
    )
    return turned.reshape(row_count, head_count * head_size).astype(jnp.bfloat16)


def owner_order(block_owner, per_device):
    block_count = block_owner.shape[0]
    blocks = jnp.arange(block_count, dtype=jnp.int32)
    same_owner = block_owner[:, None] == block_owner[None, :]
    earlier = blocks[None, :] < blocks[:, None]
    owner_rank = jnp.sum((same_owner & earlier).astype(jnp.int32), axis=1)
    target = block_owner * per_device + owner_rank
    return jnp.sum(jnp.where(target[None, :] == blocks[:, None], blocks[None, :], 0), axis=1)


def relayout(local_rows, block_order):
    cp_size = lax.axis_size("cp")
    row_count, row_width = local_rows.shape
    per_device = row_count // BLOCK
    portion = BLOCK // cp_size
    pieces = local_rows.reshape(per_device, cp_size, portion * row_width)
    spread = lax.all_to_all(pieces, "cp", split_axis=1, concat_axis=0, tiled=True)
    spread = spread.reshape(per_device * cp_size, portion * row_width)
    wanted = block_order.reshape(cp_size, per_device).T.reshape(-1)
    outgoing = jnp.take(spread, wanted, axis=0).reshape(per_device, cp_size, portion * row_width)
    arrived = lax.all_to_all(outgoing, "cp", split_axis=1, concat_axis=1, tiled=True)
    return arrived.reshape(row_count, row_width)


def project(local_rows, query_weight, key_matrix, value_matrix):
    weight_list = (query_weight, key_matrix, value_matrix)
    portion = lax.all_gather(local_rows, "tp", axis=1, tiled=True)
    return tuple(
        (jnp.dot(portion, weight, preferred_element_type=jnp.float32) for weight in weight_list)
    )


def attend(queries, query_tokens, key_rows, value_rows, key_tokens, bounds, head_size, kv_heads):
    row_count = queries.shape[0]
    query_group_width = queries.shape[1] // (kv_heads * head_size)
    grouped = queries.reshape(row_count, kv_heads, query_group_width, head_size).transpose(
        1, 2, 0, 3
    )
    grouped = grouped.reshape(kv_heads, query_group_width * row_count, head_size)
    query_documents = document_of(query_tokens, bounds)
    score_scale = 1.0 / math.sqrt(head_size)

    def update(flash_state, key_block, value_block, token_block):
        block_rows = key_block.shape[0]
        key_documents = document_of(token_block, bounds)
        allowed = (query_documents[:, None] == key_documents[None, :]) & (
            token_block[None, :] <= query_tokens[:, None]
        )
        running_max, running_sum, running_out = flash_state
        per_head_keys = key_block.reshape(block_rows, kv_heads, head_size).transpose(1, 0, 2)
        per_head_values = value_block.reshape(block_rows, kv_heads, head_size).transpose(1, 0, 2)
        scores = (
            jnp.einsum("khd,ksd->khs", grouped, per_head_keys, preferred_element_type=jnp.float32)
            * score_scale
        )
        wide_mask = jnp.tile(allowed, (query_group_width, 1))[None, :, :]
        scores = jnp.where(wide_mask, scores, masked_score)
        new_max = jnp.maximum(running_max, jnp.max(scores, axis=2))
        weights = jnp.where(wide_mask, jnp.exp(scores - new_max[:, :, None]), 0.0)
        factor = jnp.exp(running_max - new_max)
        new_sum = running_sum * factor + jnp.sum(weights, axis=2)
        new_out = running_out * factor[:, :, None] + jnp.einsum(
            "khs,ksd->khd",
            weights.astype(jnp.bfloat16),
            per_head_values,
            preferred_element_type=jnp.float32,
        )
        return (new_max, new_sum, new_out)

    initial = (
        jnp.full((kv_heads, query_group_width * row_count), masked_score, jnp.float32),
        jnp.zeros((kv_heads, query_group_width * row_count), jnp.float32),
        jnp.zeros((kv_heads, query_group_width * row_count, head_size), jnp.float32),
    )
    key_part = lax.all_gather(key_rows, "cp", axis=0, tiled=True)
    value_part = lax.all_gather(value_rows, "cp", axis=0, tiled=True)
    token_part = lax.all_gather(key_tokens, "cp", axis=0, tiled=True)
    part_rows = key_part.shape[0]
    block_rows = math.gcd(part_rows, 512)

    def one_block(block_index, inner_state):
        first_row = block_index * block_rows
        return update(
            inner_state,
            lax.dynamic_slice_in_dim(key_part, first_row, block_rows, 0),
            lax.dynamic_slice_in_dim(value_part, first_row, block_rows, 0),
            lax.dynamic_slice_in_dim(token_part, first_row, block_rows, 0),
        )

    final_max, final_sum, final_out = lax.fori_loop(0, part_rows // block_rows, one_block, initial)
    normalized = final_out / final_sum[:, :, None]
    merged = normalized.reshape(kv_heads, query_group_width, row_count, head_size).transpose(
        2, 0, 1, 3
    )
    return merged.reshape(row_count, kv_heads * query_group_width * head_size).astype(jnp.bfloat16)


def output_rows(heads_out, output_weight):
    head_terms = jnp.dot(heads_out, output_weight, preferred_element_type=jnp.float32)
    return lax.psum_scatter(head_terms.astype(jnp.bfloat16), "tp", scatter_dimension=1, tiled=True)


MESH = pl.DeviceIdType.MESH
VMEM_LIMIT = 53 << 20
PASS_ROWS = 128
LEAD = 3


def dot(a, b):
    return jnp.dot(a, b, preferred_element_type=jnp.float32)


def fill_rows(x):
    copies = max(PASS_ROWS // x.shape[0], 1)
    return jnp.concatenate([x] * copies, axis=0) if copies > 1 else x


def turn(raw, cosine, sine):
    half = raw.shape[1] // 2
    swapped = jnp.concatenate([raw[:, half:], raw[:, :half]], axis=1)
    return (raw * cosine + swapped * sine).astype(jnp.bfloat16)


def greet(n_cp, n_tp):
    c, z = lax.axis_index("cp"), lax.axis_index("tp")
    barrier = pltpu.get_barrier_semaphore()
    for t in range(1, n_cp):
        peer = lax.rem(c + t, n_cp)
        pl.semaphore_signal(barrier, inc=1, device_id={"cp": peer}, device_id_type=MESH)
    for t in range(1, n_tp):
        peer = lax.rem(z + t, n_tp)
        pl.semaphore_signal(barrier, inc=1, device_id={"tp": peer}, device_id_type=MESH)
    pl.semaphore_wait(barrier, n_cp + n_tp - 2)


def row_tokens(bounds, blocks, share, offset):
    shape = (blocks, share, HEAD_WIDTH)
    token = (
        lax.broadcasted_iota(jnp.int32, shape, 0) * BLOCK
        + lax.broadcasted_iota(jnp.int32, shape, 1) + offset
    )
    start = jnp.zeros_like(token)
    for i in range(len(bounds) - 1):
        start = jnp.where(token >= bounds[i], bounds[i], start)
    return token, start


def chunk_sizes(sources):
    if sources < 4 or sources % 2:
        return [1] * sources
    return [2] * ((sources - 2) // 2) + [1, 1]


def fused_kernel(
    n_cp, n_tp, sizes, bound_count,
    table, hidden, wq_hbm, wk_hbm, wv_hbm, wo_hbm, inverse,
    out_ref,
    rows, w, wo, cosine, sine, tokens, starts, q_all, kv_own, kv_all,
    part, from_left, from_right, to_right, to_left, done, outgoing, landed, order,
    w_sem, o_sem, own_sem, s_send, s_recv, r_send, l_send, z_recv, k_send, k_recv,
    pr_send, pl_send, pr_recv, pl_recv, a_send, a_recv,
):
    c, z = lax.axis_index("cp"), lax.axis_index("tp")
    bounds = [table[i] for i in range(bound_count)]
    owner = [table[bound_count + b] for b in range(table.shape[0] - bound_count)]
    per, share, width = hidden.shape[0], hidden.shape[2], hidden.shape[3]
    blocks = per * n_cp
    unit = per * share
    q_width = wq_hbm.shape[1]
    heads = q_width // HEAD_WIDTH
    end = n_tp - 1
    last = len(sizes)
    firsts = [sum(sizes[:k]) for k in range(last + 1)]
    factor_of = math.log2(math.e) / math.sqrt(HEAD_WIDTH)
    weights = (
        pltpu.make_async_copy(wk_hbm, w.at[:, pl.ds(q_width, HEAD_WIDTH)], w_sem),
        pltpu.make_async_copy(wv_hbm, w.at[:, pl.ds(q_width + HEAD_WIDTH, HEAD_WIDTH)], w_sem),
        pltpu.make_async_copy(wq_hbm, w.at[:, pl.ds(0, q_width)], w_sem),
    )

    def out_weight(o):
        return pltpu.make_async_copy(
            wo_hbm.at[:, pl.ds(o * width, width)], wo.at[o], o_sem
        )

    own = pltpu.make_async_copy(hidden.at[:, c], rows.at[z, pl.ds(c * per, per)], own_sem)
    own.start()
    greet(n_cp, n_tp)

    def spread(i):
        peer = lax.rem(c + i, n_cp)
        return pltpu.make_async_remote_copy(
            src_ref=hidden.at[:, peer], dst_ref=rows.at[z, pl.ds(c * per, per)],
            send_sem=s_send, recv_sem=s_recv.at[i],
            device_id={"cp": peer}, device_id_type=MESH,
        )

    def along(origin, source, step):
        piece = rows.at[origin, pl.ds(source * per, per)]
        sems = r_send if step > 0 else l_send
        return pltpu.make_async_remote_copy(
            src_ref=piece, dst_ref=piece,
            send_sem=sems, recv_sem=z_recv.at[origin, source],
            device_id={"tp": lax.rem(z + step + n_tp, n_tp)}, device_id_type=MESH,
        )

    def blocks_of(k):
        return pl.ds(firsts[k] * per, sizes[k] * per)

    def lines_of(k):
        return pl.ds(firsts[k] * unit, sizes[k] * unit)

    def keys_to(i, k):
        return pltpu.make_async_remote_copy(
            src_ref=kv_own.at[blocks_of(k)], dst_ref=kv_all.at[blocks_of(k), c],
            send_sem=k_send, recv_sem=k_recv.at[k],
            device_id={"cp": lax.rem(c + i, n_cp)}, device_id_type=MESH,
        )

    def rightward(o, k):
        return pltpu.make_async_remote_copy(
            src_ref=to_right.at[o, lines_of(k)], dst_ref=from_left.at[o, lines_of(k)],
            send_sem=pr_send, recv_sem=pr_recv.at[o - 1, k],
            device_id={"tp": lax.rem(z + 1, n_tp)}, device_id_type=MESH,
        )

    def leftward(o, k):
        return pltpu.make_async_remote_copy(
            src_ref=to_left.at[o, lines_of(k)], dst_ref=from_right.at[o, lines_of(k)],
            send_sem=pl_send, recv_sem=pl_recv.at[o, k],
            device_id={"tp": lax.rem(z + n_tp - 1, n_tp)}, device_id_type=MESH,
        )

    def final(i):
        peer = lax.rem(c + i, n_cp)
        return pltpu.make_async_remote_copy(
            src_ref=outgoing.at[pl.ds(peer * per, per)], dst_ref=landed.at[:, c],
            send_sem=a_send, recv_sem=a_recv,
            device_id={"cp": peer}, device_id_type=MESH,
        )

    for i in range(1, n_cp):
        spread(i).start()
    for copy in weights:
        copy.start()
    for o in range(n_tp):
        out_weight(o).start()

    token, start = row_tokens(bounds, blocks, share, c * share)
    tokens[...] = token.reshape(-1, HEAD_WIDTH)
    starts[...] = start.reshape(-1, HEAD_WIDTH)
    angle = (token - start).astype(jnp.float32).reshape(-1, HEAD_WIDTH) * inverse[...]
    cosine[...] = jnp.cos(angle)
    lane = lax.broadcasted_iota(jnp.int32, angle.shape, 1)
    sine[...] = jnp.where(lane < HEAD_WIDTH // 2, -1.0, 1.0) * jnp.sin(angle)
    slots = []
    for b in range(blocks):
        rank = jnp.int32(0)
        for e in range(b):
            rank += (owner[e] == owner[b]).astype(jnp.int32)
        slots.append(owner[b] * per + rank)
    for b in range(blocks):
        found = jnp.int32(0)
        for e in range(1, blocks):
            found = jnp.where(slots[e] == b, e, found)
        order[b] = found
    own.wait()

    inner = (z > 0) & (z < end)

    def take(source):
        @pl.when(source != c)
        def _():
            spread(lax.rem(c - source + n_cp, n_cp)).wait_recv()

    def end_sends(source):
        @pl.when(z == 0)
        def _():
            along(z, source, 1).start()

        @pl.when(z == end)
        def _():
            along(z, source, -1).start()

    def end_waits(source):
        for d in range(1, n_tp):
            @pl.when(z == end)
            def _():
                along(z - d, source, 1).wait_recv()

            @pl.when(z == 0)
            def _():
                along(z + d, source, -1).wait_recv()

    def flow(source, d, near):
        if source >= n_cp:
            return
        rights = (z == end - 1) if near else (z < end - 1)
        lefts = (z == 1) if near else (z > 1)

        @pl.when(inner & rights & (z - d >= 0))
        def _():
            if d > 0:
                along(z - d, source, 1).wait_recv()
            along(z - d, source, 1).start()

        @pl.when(inner & lefts & (z + d < n_tp))
        def _():
            if d > 0:
                along(z + d, source, -1).wait_recv()
            along(z + d, source, -1).start()

    def far(source):
        with jax.named_scope("far"):
            for d in range(1, end):
                flow(source, d, False)
            flow(source + 1, 0, False)

    def near(source):
        with jax.named_scope("near"):
            for d in range(1, end):
                flow(source, d, True)
            flow(source + 2, 0, True)

    def ends(source):
        with jax.named_scope("ends"):
            end_waits(source)

    def project(k):
        count = sizes[k] * unit
        x = jnp.concatenate(
            [rows[o, blocks_of(k)].reshape(count, width) for o in range(n_tp)], axis=1
        )
        cos_t, sin_t = cosine[lines_of(k), :], sine[lines_of(k), :]
        x = fill_rows(x)
        raw = dot(x, w[:, q_width:])[:count]
        key = turn(raw[:, :HEAD_WIDTH], cos_t, sin_t)
        value = raw[:, HEAD_WIDTH:].astype(jnp.bfloat16)
        tile = jnp.concatenate([key, value], axis=1)
        tile = tile.reshape(sizes[k] * per, share, 2 * HEAD_WIDTH)
        kv_own[blocks_of(k)] = tile
        kv_all[blocks_of(k), pl.ds(c, 1)] = tile[:, None]
        for i in range(1, n_cp):
            keys_to(i, k).start()
        raw_q = dot(x, w[:, :q_width])[:count]
        for h in range(heads):
            q_all[pl.ds(firsts[k] * unit * heads + h * count, count), :] = turn(
                raw_q[:, h * HEAD_WIDTH : (h + 1) * HEAD_WIDTH], cos_t, sin_t
            )

    def attend(k):
        count = sizes[k] * unit
        q = q_all[pl.ds(firsts[k] * unit * heads, heads * count), :]
        start = jnp.tile(starts[lines_of(k), :], (heads, 1))[:, :1]
        token = jnp.tile(tokens[lines_of(k), :], (heads, 1))[:, :1]

        def scored(source, size, diagonal):
            keys = size * per * BLOCK
            span = pl.ds(source * per, size * per)
            key = kv_all[span, :, :, :HEAD_WIDTH].reshape(keys, HEAD_WIDTH)
            value = kv_all[span, :, :, HEAD_WIDTH:].reshape(keys, HEAD_WIDTH)
            score = lax.dot_general(
                q, key, (((1,), (1,)), ((), ())), preferred_element_type=jnp.float32
            )
            index = source * (per * BLOCK) + lax.broadcasted_iota(jnp.int32, score.shape, 1)
            allowed = index >= start
            if diagonal:
                allowed = allowed & (index <= token)
            return jnp.where(allowed, score, masked_score), value

        def lane_sums(weight):
            partial = weight[:, :HEAD_WIDTH]
            for g in range(1, weight.shape[1] // HEAD_WIDTH):
                partial = partial + weight[:, g * HEAD_WIDTH : (g + 1) * HEAD_WIDTH]
            return partial

        def more(source, size, diagonal, carry):
            top, total, out = carry
            score, value = scored(source, size, diagonal)
            new_top = jnp.maximum(top, jnp.max(score, axis=1, keepdims=True))
            weight = jnp.exp2((score - new_top) * factor_of)
            factor = jnp.exp2((top - new_top) * factor_of)
            total = total * factor + lane_sums(weight)
            out = out * factor + dot(weight.astype(jnp.bfloat16), value)
            return new_top, total, out

        lengths = (heads * count, 1)
        carry = (
            jnp.full(lengths, masked_score, jnp.float32),
            jnp.zeros((heads * count, HEAD_WIDTH), jnp.float32),
            jnp.zeros((heads * count, HEAD_WIDTH), jnp.float32),
        )
        pairs = firsts[k] // 2
        if pairs > 0:
            carry = lax.fori_loop(0, pairs, lambda j, held: more(2 * j, 2, False, held), carry)
        if firsts[k] % 2:
            carry = more(firsts[k] - 1, 1, False, carry)
        with jax.named_scope("kvwait"):
            arrive(k)
        carry = more(firsts[k], sizes[k], True, carry)
        _, total, out = carry
        out = (out / jnp.sum(total, axis=1, keepdims=True)).astype(jnp.bfloat16)
        return jnp.concatenate([out[h * count : (h + 1) * count] for h in range(heads)], axis=1)

    def output(k, attended):
        high = z // (n_tp // 2)
        count = attended.shape[0]
        attended = fill_rows(attended)
        for turn_of in range(n_tp):
            o = (1 - high) * (end - turn_of) + high * turn_of
            product = dot(attended, wo[o])[:count]
            go_right = (z == 0) & (o > z)
            go_left = (z == end) & (o < z)

            @pl.when(go_right)
            def _():
                to_right[o, lines_of(k)] = product.astype(jnp.bfloat16)

            @pl.when(go_left)
            def _():
                to_left[o, lines_of(k)] = product.astype(jnp.bfloat16)

            @pl.when(go_right & (o > z + 1))
            def _():
                rightward(o, k).start()

            @pl.when(go_left & (o < z - 1))
            def _():
                leftward(o, k).start()

            @pl.when(jnp.logical_not(go_right | go_left))
            def _():
                part[o, lines_of(k)] = product

    def adjacent(k):
        @pl.when(z == 0)
        def _():
            rightward(1, k).start()

        @pl.when(z == end)
        def _():
            leftward(end - 1, k).start()

    def hop(k, h, dests):
        lines = lines_of(k)

        @pl.when(z == h)
        def _():
            for o in list(range(end, h, -1))[dests]:
                rightward(o, k).wait_recv()
                total = part[o, lines] + from_left[o, lines].astype(jnp.float32)
                to_right[o, lines] = total.astype(jnp.bfloat16)
                rightward(o, k).start()

        @pl.when(z == end - h)
        def _():
            for o in list(range(end - h))[dests]:
                leftward(o, k).wait_recv()
                total = part[o, lines] + from_right[o, lines].astype(jnp.float32)
                to_left[o, lines] = total.astype(jnp.bfloat16)
                leftward(o, k).start()

    def finish(k):
        lines = lines_of(k)

        @pl.when(z > 0)
        def _():
            rightward(z, k).wait_recv()
            part[z, lines] += from_left[z, lines].astype(jnp.float32)

        @pl.when(z < end)
        def _():
            leftward(z, k).wait_recv()
            part[z, lines] += from_right[z, lines].astype(jnp.float32)

        summed = part[z, lines].astype(jnp.bfloat16)
        done[blocks_of(k)] = summed.reshape(sizes[k] * per, share, width)

    def arrive(k):
        landed_keys = kv_all.at[blocks_of(k), pl.ds(0, n_cp - 1)]
        pltpu.make_async_copy(landed_keys, landed_keys, k_recv.at[k]).wait()

    def reduce(k, h, dests=slice(None)):
        with jax.named_scope(f"reduce{k}{h}"):
            hop(k, h, dests)

    with jax.named_scope("fill"):
        for source in range(n_cp):
            take(source)
            end_sends(source)
            if source < 2:
                flow(source, 0, False)
            if source < LEAD:
                flow(source, 0, True)
        for source in range(LEAD):
            for d in range(1, end):
                flow(source, d, False)
            if source == 0:
                flow(2, 0, False)
            if source == LEAD - 1:
                for d in range(2, end):
                    flow(0, d, True)
            if end > 1:
                flow(source, 1, True)
        for source in range(1, LEAD):
            for d in range(2, end):
                flow(source, d, True)
        flow(LEAD, 0, True)
        flow(LEAD, 0, False)
        far(LEAD)
        flow(LEAD + 1, 0, True)
        ends(0)
    pltpu.make_async_copy(w, w, w_sem).wait()
    passed, reached = LEAD, LEAD - 1

    def pass_on(fars, nears):
        nonlocal passed, reached
        while passed < min(fars, n_cp - 1):
            passed += 1
            far(passed)
        while reached < min(nears, n_cp - 1):
            reached += 1
            near(reached)

    parts = (slice(0, 1), slice(1, None))
    hops = [(k, h, p) for k in range(last) for h in range(1, end) for p in range(2)]
    held = {}

    def run(k, h, *wanted):
        for p in wanted:
            if (k, h, p) in hops:
                hops.remove((k, h, p))
                reduce(k, h, parts[p])

    def projection(k):
        pass_on(0, firsts[k + 1] - 1)
        for source in range(max(firsts[k], 1), firsts[k + 1]):
            ends(source)
        with jax.named_scope("project"):
            project(k)

    def attention(k):
        with jax.named_scope("attend"):
            held[k] = attend(k)

    def result(k):
        with jax.named_scope("output"):
            output(k, held.pop(k))

    def adjacents(*chosen):
        for k in chosen:
            adjacent(k)

    if last == 5:
        plan = [
            (projection, 0), (pass_on, 5, 3), (attention, 0), (pass_on, 6, 4),
            (result, 0), (adjacents, 0),
            (projection, 1), (pass_on, n_cp, 6), (attention, 1), (pass_on, n_cp, n_cp),
            (result, 1), (adjacents, 1), (run, 0, 1, 0, 1),
            (projection, 2), (projection, 3), (attention, 2), (run, 1, 1, 0),
            (result, 2), (run, 1, 1, 1), (run, 0, 2, 0, 1),
            (projection, 4), (attention, 3), (run, 2, 1, 0), (result, 3), (run, 2, 1, 1),
            (run, 1, 2, 0, 1), (attention, 4), (run, 3, 1, 0), (result, 4), (adjacents, 2, 3, 4),
            (run, 3, 1, 1), (run, 2, 2, 0, 1), (run, 4, 1, 0), (run, 3, 2, 0, 1),
        ]
    else:
        plan = []
        for k in range(last):
            plan += [(projection, k), (pass_on, n_cp, n_cp), (attention, k), (result, k), (adjacents, k)]
    pltpu.make_async_copy(wo, wo, o_sem).wait()
    for step, *given in plan:
        step(*given)
    for k, h, p in list(hops):
        reduce(k, h, parts[p])
    with jax.named_scope("finish"):
        for k in range(last):
            finish(k)

    with jax.named_scope("a2a"):
        for b in range(blocks):
            outgoing[b] = done[order[b]]
        for i in range(1, n_cp):
            final(i).start()
        out_ref[:, pl.ds(c, 1)] = outgoing[pl.ds(c * per, per)][:, None]
        others = landed.at[:, pl.ds(0, n_cp - 1)]
        pltpu.make_async_copy(others, others, a_recv).wait()
        for i in range(1, n_cp):
            source = lax.rem(c - i + n_cp, n_cp)
            out_ref[:, pl.ds(source, 1)] = landed[:, pl.ds(source, 1)]

    def drain(ref, sem):
        pltpu.make_async_copy(ref, ref, sem).wait()

    drain(landed.at[:, pl.ds(0, n_cp - 1)], s_send)
    drain(landed.at[:, pl.ds(0, n_cp - 1)], a_send)
    drain(kv_all.at[:, pl.ds(0, n_cp - 1)], k_send)
    for v in range(n_tp):
        @pl.when(z == v)
        def _():
            if v < end:
                drain(rows.at[pl.ds(0, v + 1)], r_send)
                drain(to_right.at[pl.ds(0, end - v)], pr_send)
            if v > 0:
                drain(rows.at[pl.ds(0, n_tp - v)], l_send)
                drain(to_left.at[pl.ds(0, v)], pl_send)


def fused_call(bounds, owner, hidden, wq, wk, wv, wo, inverse, n_cp, n_tp):
    rows, width = hidden.shape
    per = rows // BLOCK
    share = BLOCK // n_cp
    blocks = per * n_cp
    heads = wq.shape[1] // HEAD_WIDTH
    sizes = chunk_sizes(n_cp)
    pieces = hidden.reshape(per, n_cp, share, width)
    bf, f32, i32, dma = jnp.bfloat16, jnp.float32, jnp.int32, pltpu.SemaphoreType.DMA
    vmem = pl.BlockSpec(memory_space=pltpu.VMEM)
    hbm = pl.BlockSpec(memory_space=pltpu.HBM)
    smem = pl.BlockSpec(memory_space=pltpu.SMEM)
    slab = (n_tp, rows, width)
    kv_width = 2 * HEAD_WIDTH
    sums = dma((n_tp - 1, len(sizes)))
    flops = 2 * rows * (wq.shape[0] * (wq.shape[1] + kv_width) + wo.shape[0] * wo.shape[1])
    out = pl.pallas_call(
        functools.partial(fused_kernel, n_cp, n_tp, sizes, bounds.shape[0]),
        out_shape=jax.ShapeDtypeStruct((per, n_cp, share, width), bf),
        in_specs=[smem, hbm, hbm, hbm, hbm, hbm, vmem],
        out_specs=vmem,
        scratch_shapes=[
            pltpu.VMEM((n_tp, blocks, share, width), bf),
            pltpu.VMEM((wq.shape[0], wq.shape[1] + kv_width), bf),
            pltpu.VMEM((n_tp, wo.shape[0], width), bf),
            pltpu.VMEM((rows, HEAD_WIDTH), f32), pltpu.VMEM((rows, HEAD_WIDTH), f32),
            pltpu.VMEM((rows, HEAD_WIDTH), i32), pltpu.VMEM((rows, HEAD_WIDTH), i32),
            pltpu.VMEM((rows * heads, HEAD_WIDTH), bf),
            pltpu.VMEM((blocks, share, kv_width), bf),
            pltpu.VMEM((blocks, n_cp, share, kv_width), bf),
            pltpu.VMEM(slab, f32),
            pltpu.VMEM(slab, bf), pltpu.VMEM(slab, bf), pltpu.VMEM(slab, bf), pltpu.VMEM(slab, bf),
            pltpu.VMEM((blocks, share, width), bf),
            pltpu.VMEM((blocks, share, width), bf),
            pltpu.VMEM((per, n_cp, share, width), bf),
            pltpu.SMEM((blocks,), i32),
            dma, dma, dma, dma, dma((n_cp,)), dma, dma, dma((n_tp, n_cp)),
            dma, dma((len(sizes),)), dma, dma, sums, sums, dma, dma,
        ],
        compiler_params=pltpu.CompilerParams(
            collective_id=1, has_side_effects=True, vmem_limit_bytes=VMEM_LIMIT
        ),
        cost_estimate=pl.CostEstimate(flops=flops, bytes_accessed=20 << 20, transcendentals=0),
    )(jnp.concatenate([bounds, owner]), pieces, wq, wk, wv, wo, inverse)
    return out.reshape(rows, width)


def local_fused(
    hidden, query_weight, key_matrix, value_matrix, output_weight, document_bounds, block_owner
):
    n_cp, n_tp = lax.axis_size("cp"), lax.axis_size("tp")
    inverse = jnp.tile(rope_inverse(HEAD_WIDTH), 2)[None, :]
    return fused_call(
        document_bounds, block_owner, hidden, query_weight, key_matrix, value_matrix,
        output_weight, inverse, n_cp, n_tp,
    )


def local_plain(
    hidden, query_weight, key_matrix, value_matrix, output_weight, document_bounds, block_owner
):
    cp_index = lax.axis_index("cp")
    row_count = hidden.shape[0]
    per_device = row_count // BLOCK
    block_order = owner_order(block_owner, per_device)
    own_blocks = lax.dynamic_slice_in_dim(block_order, cp_index * per_device, per_device, 0)
    new_tokens = (
        own_blocks[:, None] * BLOCK + jnp.arange(BLOCK, dtype=jnp.int32)[None, :]
    ).reshape(-1)
    kv_heads = key_matrix.shape[1] // HEAD_WIDTH
    moved = relayout(hidden, block_order)
    query_raw, key_raw, value_raw = project(moved, query_weight, key_matrix, value_matrix)
    queries = rotate(query_raw, new_tokens, document_bounds, HEAD_WIDTH)
    key_rows = rotate(key_raw, new_tokens, document_bounds, HEAD_WIDTH)
    value_rows = value_raw.astype(jnp.bfloat16)
    heads_out = attend(
        queries, new_tokens, key_rows, value_rows, new_tokens, document_bounds, HEAD_WIDTH, kv_heads
    )
    return output_rows(heads_out, output_weight)


def solution(mesh):
    shares = BLOCK // mesh.shape["cp"]
    local = local_fused if shares % 16 == 0 else local_plain
    placed = (P("cp", "tp"), P(None, "tp"), P(None, "tp"), P(None, "tp"), P("tp", None), P(), P())
    return jax.shard_map(
        local, mesh=mesh, in_specs=placed, out_specs=P("cp", "tp"), check_vma=False
    )
```

```python
import functools
import math

import jax
import jax.numpy as jnp
from jax import lax
from jax.experimental import pallas as pl
from jax.experimental.pallas import tpu as pltpu
from jax.sharding import PartitionSpec as P

HEAD_WIDTH = 128
BLOCK = 128


rope_theta = 500000.0
rope_factor = 8.0
rope_context = 8192.0
masked_score = -1e30


def rope_inverse(head_size):
    halves = jnp.arange(head_size // 2, dtype=jnp.float32)
    inverse = 1.0 / rope_theta ** (2.0 * halves / head_size)
    wavelength = 2.0 * math.pi / inverse
    smooth = (rope_context / wavelength - 1.0) / 3.0
    blended = (1.0 - smooth) * inverse / rope_factor + smooth * inverse
    longer = jnp.where(wavelength > rope_context, inverse / rope_factor, blended)
    return jnp.where(wavelength < rope_context / 4.0, inverse, longer)


def document_of(tokens, bounds):
    inner_bounds = bounds[1:-1]
    return jnp.sum((tokens[:, None] >= inner_bounds[None, :]).astype(jnp.int32), axis=1)


def position_of(tokens, bounds):
    starts = bounds[:-1]
    document_start = jnp.max(
        jnp.where(starts[None, :] <= tokens[:, None], starts[None, :], 0), axis=1
    )
    return tokens - document_start


def rotate(raw_rows, tokens, bounds, head_size):
    row_count = raw_rows.shape[0]
    head_count = raw_rows.shape[1] // head_size
    angles = (
        position_of(tokens, bounds).astype(jnp.float32)[:, None] * rope_inverse(head_size)[None, :]
    )
    cosine = jnp.cos(angles)[:, None, :]
    sine_table = jnp.sin(angles)[:, None, :]
    heads_view = raw_rows.reshape(row_count, head_count, head_size)
    front_half = heads_view[:, :, : head_size // 2]
    back_half = heads_view[:, :, head_size // 2 :]
    turned = jnp.concatenate(
        [
            front_half * cosine - back_half * sine_table,
            back_half * cosine + front_half * sine_table,
        ],
        axis=2,
    )
    return turned.reshape(row_count, head_count * head_size).astype(jnp.bfloat16)


def owner_order(block_owner, per_device):
    block_count = block_owner.shape[0]
    blocks = jnp.arange(block_count, dtype=jnp.int32)
    same_owner = block_owner[:, None] == block_owner[None, :]
    earlier = blocks[None, :] < blocks[:, None]
    owner_rank = jnp.sum((same_owner & earlier).astype(jnp.int32), axis=1)
    target = block_owner * per_device + owner_rank
    return jnp.sum(jnp.where(target[None, :] == blocks[:, None], blocks[None, :], 0), axis=1)


def relayout(local_rows, block_order):
    cp_size = lax.axis_size("cp")
    row_count, row_width = local_rows.shape
    per_device = row_count // BLOCK
    portion = BLOCK // cp_size
    pieces = local_rows.reshape(per_device, cp_size, portion * row_width)
    spread = lax.all_to_all(pieces, "cp", split_axis=1, concat_axis=0, tiled=True)
    spread = spread.reshape(per_device * cp_size, portion * row_width)
    wanted = block_order.reshape(cp_size, per_device).T.reshape(-1)
    outgoing = jnp.take(spread, wanted, axis=0).reshape(per_device, cp_size, portion * row_width)
    arrived = lax.all_to_all(outgoing, "cp", split_axis=1, concat_axis=1, tiled=True)
    return arrived.reshape(row_count, row_width)


def project(local_rows, query_weight, key_matrix, value_matrix):
    weight_list = (query_weight, key_matrix, value_matrix)
    portion = lax.all_gather(local_rows, "tp", axis=1, tiled=True)
    return tuple(
        (jnp.dot(portion, weight, preferred_element_type=jnp.float32) for weight in weight_list)
    )


def attend(queries, query_tokens, key_rows, value_rows, key_tokens, bounds, head_size, kv_heads):
    row_count = queries.shape[0]
    query_group_width = queries.shape[1] // (kv_heads * head_size)
    grouped = queries.reshape(row_count, kv_heads, query_group_width, head_size).transpose(
        1, 2, 0, 3
    )
    grouped = grouped.reshape(kv_heads, query_group_width * row_count, head_size)
    query_documents = document_of(query_tokens, bounds)
    score_scale = 1.0 / math.sqrt(head_size)

    def update(flash_state, key_block, value_block, token_block):
        block_rows = key_block.shape[0]
        key_documents = document_of(token_block, bounds)
        allowed = (query_documents[:, None] == key_documents[None, :]) & (
            token_block[None, :] <= query_tokens[:, None]
        )
        running_max, running_sum, running_out = flash_state
        per_head_keys = key_block.reshape(block_rows, kv_heads, head_size).transpose(1, 0, 2)
        per_head_values = value_block.reshape(block_rows, kv_heads, head_size).transpose(1, 0, 2)
        scores = (
            jnp.einsum("khd,ksd->khs", grouped, per_head_keys, preferred_element_type=jnp.float32)
            * score_scale
        )
        wide_mask = jnp.tile(allowed, (query_group_width, 1))[None, :, :]
        scores = jnp.where(wide_mask, scores, masked_score)
        new_max = jnp.maximum(running_max, jnp.max(scores, axis=2))
        weights = jnp.where(wide_mask, jnp.exp(scores - new_max[:, :, None]), 0.0)
        factor = jnp.exp(running_max - new_max)
        new_sum = running_sum * factor + jnp.sum(weights, axis=2)
        new_out = running_out * factor[:, :, None] + jnp.einsum(
            "khs,ksd->khd",
            weights.astype(jnp.bfloat16),
            per_head_values,
            preferred_element_type=jnp.float32,
        )
        return (new_max, new_sum, new_out)

    initial = (
        jnp.full((kv_heads, query_group_width * row_count), masked_score, jnp.float32),
        jnp.zeros((kv_heads, query_group_width * row_count), jnp.float32),
        jnp.zeros((kv_heads, query_group_width * row_count, head_size), jnp.float32),
    )
    key_part = lax.all_gather(key_rows, "cp", axis=0, tiled=True)
    value_part = lax.all_gather(value_rows, "cp", axis=0, tiled=True)
    token_part = lax.all_gather(key_tokens, "cp", axis=0, tiled=True)
    part_rows = key_part.shape[0]
    block_rows = math.gcd(part_rows, 512)

    def one_block(block_index, inner_state):
        first_row = block_index * block_rows
        return update(
            inner_state,
            lax.dynamic_slice_in_dim(key_part, first_row, block_rows, 0),
            lax.dynamic_slice_in_dim(value_part, first_row, block_rows, 0),
            lax.dynamic_slice_in_dim(token_part, first_row, block_rows, 0),
        )

    final_max, final_sum, final_out = lax.fori_loop(0, part_rows // block_rows, one_block, initial)
    normalized = final_out / final_sum[:, :, None]
    merged = normalized.reshape(kv_heads, query_group_width, row_count, head_size).transpose(
        2, 0, 1, 3
    )
    return merged.reshape(row_count, kv_heads * query_group_width * head_size).astype(jnp.bfloat16)


def output_rows(heads_out, output_weight):
    head_terms = jnp.dot(heads_out, output_weight, preferred_element_type=jnp.float32)
    return lax.psum_scatter(head_terms.astype(jnp.bfloat16), "tp", scatter_dimension=1, tiled=True)


MESH = pl.DeviceIdType.MESH
VMEM_LIMIT = 53 << 20
PASS_ROWS = 128
LEAD = 3


def dot(a, b):
    return jnp.dot(a, b, preferred_element_type=jnp.float32)


def fill_rows(x):
    copies = max(PASS_ROWS // x.shape[0], 1)
    return jnp.concatenate([x] * copies, axis=0) if copies > 1 else x


def turn(raw, cosine, sine):
    half = raw.shape[1] // 2
    swapped = jnp.concatenate([raw[:, half:], raw[:, :half]], axis=1)
    return (raw * cosine + swapped * sine).astype(jnp.bfloat16)


def greet(n_cp, n_tp):
    c, z = lax.axis_index("cp"), lax.axis_index("tp")
    barrier = pltpu.get_barrier_semaphore()
    for t in range(1, n_cp):
        peer = lax.rem(c + t, n_cp)
        pl.semaphore_signal(barrier, inc=1, device_id={"cp": peer}, device_id_type=MESH)
    for t in range(1, n_tp):
        peer = lax.rem(z + t, n_tp)
        pl.semaphore_signal(barrier, inc=1, device_id={"tp": peer}, device_id_type=MESH)
    pl.semaphore_wait(barrier, n_cp + n_tp - 2)


def row_tokens(bounds, blocks, share, offset):
    shape = (blocks, share, HEAD_WIDTH)
    token = (
        lax.broadcasted_iota(jnp.int32, shape, 0) * BLOCK
        + lax.broadcasted_iota(jnp.int32, shape, 1) + offset
    )
    start = jnp.zeros_like(token)
    for i in range(len(bounds) - 1):
        start = jnp.where(token >= bounds[i], bounds[i], start)
    return token, start


def chunk_sizes(sources):
    if sources < 4 or sources % 2:
        return [1] * sources
    return [2] * (sources // 2)


def fused_kernel(
    n_cp, n_tp, sizes, bound_count,
    table, hidden, wq_hbm, wk_hbm, wv_hbm, wo_hbm, inverse,
    out_ref,
    mine, rows, w, wo, cosine, sine, tokens, starts, q_all, kv_own, kv_all,
    part, from_left, from_right, to_right, to_left, done, outgoing, landed, order,
    w_sem, o_sem, own_sem, m_sem, s_send, s_recv, r_send, l_send, z_recv, k_send, k_recv,
    pr_send, pl_send, pr_recv, pl_recv, a_send, a_recv,
):
    c, z = lax.axis_index("cp"), lax.axis_index("tp")
    bounds = [table[i] for i in range(bound_count)]
    owner = [table[bound_count + b] for b in range(table.shape[0] - bound_count)]
    per, share, width = hidden.shape[0], hidden.shape[2], hidden.shape[3]
    blocks = per * n_cp
    unit = per * share
    q_width = wq_hbm.shape[1]
    heads = q_width // HEAD_WIDTH
    end = n_tp - 1
    last = len(sizes)
    firsts = [sum(sizes[:k]) for k in range(last + 1)]
    spans = [(firsts[k] * unit, sizes[k] * unit) for k in range(last - 1)]
    spans += [(firsts[last - 1] * unit + b * share, share) for b in range(sizes[-1] * per)]
    units_of = [[k] for k in range(last - 1)] + [list(range(last - 1, len(spans)))]
    groups = [[(a, 1) for a in range(firsts[k], firsts[k + 1])] for k in range(last)]
    factor_of = math.log2(math.e) / math.sqrt(HEAD_WIDTH)
    weights = (
        pltpu.make_async_copy(wk_hbm, w.at[:, pl.ds(q_width, HEAD_WIDTH)], w_sem),
        pltpu.make_async_copy(wv_hbm, w.at[:, pl.ds(q_width + HEAD_WIDTH, HEAD_WIDTH)], w_sem),
        pltpu.make_async_copy(wq_hbm, w.at[:, pl.ds(0, q_width)], w_sem),
    )

    def out_weight(o):
        return pltpu.make_async_copy(
            wo_hbm.at[:, pl.ds(o * width, width)], wo.at[o], o_sem
        )

    own = pltpu.make_async_copy(hidden.at[:, c], rows.at[z, pl.ds(c * per, per)], own_sem)
    staged = pltpu.make_async_copy(hidden, mine, m_sem)
    staged.start()
    own.start()
    greet(n_cp, n_tp)
    staged.wait()

    def spread(i):
        peer = lax.rem(c + i, n_cp)
        return pltpu.make_async_remote_copy(
            src_ref=mine.at[:, peer], dst_ref=rows.at[z, pl.ds(c * per, per)],
            send_sem=s_send, recv_sem=s_recv.at[i],
            device_id={"cp": peer}, device_id_type=MESH,
        )

    def along(origin, source, step):
        piece = rows.at[origin, pl.ds(source * per, per)]
        sems = r_send if step > 0 else l_send
        return pltpu.make_async_remote_copy(
            src_ref=piece, dst_ref=piece,
            send_sem=sems, recv_sem=z_recv.at[origin, source],
            device_id={"tp": lax.rem(z + step + n_tp, n_tp)}, device_id_type=MESH,
        )

    def blocks_of(k):
        return pl.ds(firsts[k] * per, sizes[k] * per)

    def lines_of(k):
        return pl.ds(firsts[k] * unit, sizes[k] * unit)

    def keys_to(i, group):
        span = pl.ds(group[0] * per, group[1] * per)
        return pltpu.make_async_remote_copy(
            src_ref=kv_own.at[span], dst_ref=kv_all.at[span, c],
            send_sem=k_send, recv_sem=k_recv.at[group[0]],
            device_id={"cp": lax.rem(c + i, n_cp)}, device_id_type=MESH,
        )

    def rightward(o, u):
        lines = pl.ds(*spans[u])
        return pltpu.make_async_remote_copy(
            src_ref=to_right.at[o, lines], dst_ref=from_left.at[o, lines],
            send_sem=pr_send, recv_sem=pr_recv.at[o - 1, u],
            device_id={"tp": lax.rem(z + 1, n_tp)}, device_id_type=MESH,
        )

    def leftward(o, u):
        lines = pl.ds(*spans[u])
        return pltpu.make_async_remote_copy(
            src_ref=to_left.at[o, lines], dst_ref=from_right.at[o, lines],
            send_sem=pl_send, recv_sem=pl_recv.at[o, u],
            device_id={"tp": lax.rem(z + n_tp - 1, n_tp)}, device_id_type=MESH,
        )

    def final(i):
        peer = lax.rem(c + i, n_cp)
        return pltpu.make_async_remote_copy(
            src_ref=outgoing.at[pl.ds(peer * per, per)], dst_ref=landed.at[:, c],
            send_sem=a_send, recv_sem=a_recv,
            device_id={"cp": peer}, device_id_type=MESH,
        )

    for i in range(1, n_cp):
        spread(i).start()
    for copy in weights:
        copy.start()
    for o in range(n_tp):
        out_weight(o).start()

    token, start = row_tokens(bounds, blocks, share, c * share)
    tokens[...] = token.reshape(-1, HEAD_WIDTH)
    starts[...] = start.reshape(-1, HEAD_WIDTH)
    angle = (token - start).astype(jnp.float32).reshape(-1, HEAD_WIDTH) * inverse[...]
    cosine[...] = jnp.cos(angle)
    lane = lax.broadcasted_iota(jnp.int32, angle.shape, 1)
    sine[...] = jnp.where(lane < HEAD_WIDTH // 2, -1.0, 1.0) * jnp.sin(angle)
    slots = []
    for b in range(blocks):
        rank = jnp.int32(0)
        for e in range(b):
            rank += (owner[e] == owner[b]).astype(jnp.int32)
        slots.append(owner[b] * per + rank)
    for b in range(blocks):
        found = jnp.int32(0)
        for e in range(1, blocks):
            found = jnp.where(slots[e] == b, e, found)
        order[b] = found
    own.wait()

    inner = (z > 0) & (z < end)

    def take(source):
        @pl.when(source != c)
        def _():
            spread(lax.rem(c - source + n_cp, n_cp)).wait_recv()

    def end_sends(source):
        @pl.when(z == 0)
        def _():
            along(z, source, 1).start()

        @pl.when(z == end)
        def _():
            along(z, source, -1).start()

    def end_waits(source):
        for d in range(1, n_tp):
            @pl.when(z == end)
            def _():
                along(z - d, source, 1).wait_recv()

            @pl.when(z == 0)
            def _():
                along(z + d, source, -1).wait_recv()

    def flow(source, d, near):
        if source >= n_cp:
            return
        rights = (z == end - 1) if near else (z < end - 1)
        lefts = (z == 1) if near else (z > 1)

        @pl.when(inner & rights & (z - d >= 0))
        def _():
            if d > 0:
                along(z - d, source, 1).wait_recv()
            along(z - d, source, 1).start()

        @pl.when(inner & lefts & (z + d < n_tp))
        def _():
            if d > 0:
                along(z + d, source, -1).wait_recv()
            along(z + d, source, -1).start()

    def far(source):
        with jax.named_scope("far"):
            for d in range(1, end):
                flow(source, d, False)
            flow(source + 1, 0, False)

    def near(source):
        with jax.named_scope("near"):
            for d in range(1, end):
                flow(source, d, True)
            if source >= LEAD:
                flow(source + 1, 0, True)

    def ends(source):
        with jax.named_scope("ends"):
            end_waits(source)

    def gathered(first, size):
        span = pl.ds(first * per, size * per)
        count = size * unit
        x = [rows[o, span].reshape(count, width) for o in range(n_tp)]
        lines = pl.ds(first * unit, count)
        return fill_rows(jnp.concatenate(x, axis=1)), cosine[lines, :], sine[lines, :]

    def project_keys(group):
        count = group[1] * unit
        span = pl.ds(group[0] * per, group[1] * per)
        x, cos_t, sin_t = gathered(*group)
        raw = dot(x, w[:, q_width:])[:count]
        key = turn(raw[:, :HEAD_WIDTH], cos_t, sin_t)
        value = raw[:, HEAD_WIDTH:].astype(jnp.bfloat16)
        tile = jnp.concatenate([key, value], axis=1)
        tile = tile.reshape(group[1] * per, share, 2 * HEAD_WIDTH)
        kv_own[span] = tile
        kv_all[span, pl.ds(c, 1)] = tile[:, None]
        for i in range(1, n_cp):
            keys_to(i, group).start()

    def project_queries(k):
        count = sizes[k] * unit
        x, cos_t, sin_t = gathered(firsts[k], sizes[k])
        raw_q = dot(x, w[:, :q_width])[:count]
        for h in range(heads):
            q_all[pl.ds(firsts[k] * unit * heads + h * count, count), :] = turn(
                raw_q[:, h * HEAD_WIDTH : (h + 1) * HEAD_WIDTH], cos_t, sin_t
            )

    def attend(k):
        count = sizes[k] * unit
        q = q_all[pl.ds(firsts[k] * unit * heads, heads * count), :]
        start = jnp.tile(starts[lines_of(k), :], (heads, 1))[:, :1]
        token = jnp.tile(tokens[lines_of(k), :], (heads, 1))[:, :1]

        def scored(source, size, diagonal):
            keys = size * per * BLOCK
            span = pl.ds(source * per, size * per)
            key = kv_all[span, :, :, :HEAD_WIDTH].reshape(keys, HEAD_WIDTH)
            value = kv_all[span, :, :, HEAD_WIDTH:].reshape(keys, HEAD_WIDTH)
            score = lax.dot_general(
                q, key, (((1,), (1,)), ((), ())), preferred_element_type=jnp.float32
            )
            index = source * (per * BLOCK) + lax.broadcasted_iota(jnp.int32, score.shape, 1)
            allowed = index >= start
            if diagonal:
                allowed = allowed & (index <= token)
            return jnp.where(allowed, score, masked_score), value

        def lane_sums(weight):
            partial = weight[:, :HEAD_WIDTH]
            for g in range(1, weight.shape[1] // HEAD_WIDTH):
                partial = partial + weight[:, g * HEAD_WIDTH : (g + 1) * HEAD_WIDTH]
            return partial

        def more(source, size, diagonal, carry):
            top, total, out = carry
            score, value = scored(source, size, diagonal)
            new_top = jnp.maximum(top, jnp.max(score, axis=1, keepdims=True))
            weight = jnp.exp2((score - new_top) * factor_of)
            factor = jnp.exp2((top - new_top) * factor_of)
            total = total * factor + lane_sums(weight)
            out = out * factor + dot(weight.astype(jnp.bfloat16), value)
            return new_top, total, out

        lengths = (heads * count, 1)
        carry = (
            jnp.full(lengths, masked_score, jnp.float32),
            jnp.zeros((heads * count, HEAD_WIDTH), jnp.float32),
            jnp.zeros((heads * count, HEAD_WIDTH), jnp.float32),
        )
        pairs = firsts[k] // 2
        if pairs > 0:
            carry = lax.fori_loop(0, pairs, lambda j, held: more(2 * j, 2, False, held), carry)
        if firsts[k] % 2:
            carry = more(firsts[k] - 1, 1, False, carry)
        with jax.named_scope("kvwait"):
            arrive(k)
        carry = more(firsts[k], sizes[k], True, carry)
        _, total, out = carry
        out = (out / jnp.sum(total, axis=1, keepdims=True)).astype(jnp.bfloat16)
        return jnp.concatenate([out[h * count : (h + 1) * count] for h in range(heads)], axis=1)

    def output(k, attended):
        high = z // (n_tp // 2)
        count = attended.shape[0]
        attended = fill_rows(attended)
        for turn_of in range(n_tp):
            o = (1 - high) * (end - turn_of) + high * turn_of
            product = dot(attended, wo[o])[:count]
            go_right = (z == 0) & (o > z)
            go_left = (z == end) & (o < z)

            @pl.when(go_right)
            def _():
                to_right[o, lines_of(k)] = product.astype(jnp.bfloat16)

            @pl.when(go_left)
            def _():
                to_left[o, lines_of(k)] = product.astype(jnp.bfloat16)

            @pl.when(go_right & (o > z + 1))
            def _():
                for u in units_of[k]:
                    rightward(o, u).start()

            @pl.when(go_left & (o < z - 1))
            def _():
                for u in units_of[k]:
                    leftward(o, u).start()

            @pl.when(jnp.logical_not(go_right | go_left))
            def _():
                part[o, lines_of(k)] = product

    def adjacent(k):
        for u in units_of[k]:
            @pl.when(z == 0)
            def _():
                rightward(1, u).start()

            @pl.when(z == end)
            def _():
                leftward(end - 1, u).start()

    def hop(u, h, dests):
        lines = pl.ds(*spans[u])

        @pl.when(z == h)
        def _():
            for o in list(range(end, h, -1))[dests]:
                rightward(o, u).wait_recv()
                total = part[o, lines] + from_left[o, lines].astype(jnp.float32)
                to_right[o, lines] = total.astype(jnp.bfloat16)
                rightward(o, u).start()

        @pl.when(z == end - h)
        def _():
            for o in list(range(end - h))[dests]:
                leftward(o, u).wait_recv()
                total = part[o, lines] + from_right[o, lines].astype(jnp.float32)
                to_left[o, lines] = total.astype(jnp.bfloat16)
                leftward(o, u).start()

    def finish(u):
        lines = pl.ds(*spans[u])

        @pl.when(z > 0)
        def _():
            rightward(z, u).wait_recv()
            part[z, lines] += from_left[z, lines].astype(jnp.float32)

        @pl.when(z < end)
        def _():
            leftward(z, u).wait_recv()
            part[z, lines] += from_right[z, lines].astype(jnp.float32)

        summed = part[z, lines].astype(jnp.bfloat16)
        taken = pl.ds(spans[u][0] // share, spans[u][1] // share)
        done[taken] = summed.reshape(spans[u][1] // share, share, width)

    def arrive(k):
        for first, size in groups[k]:
            keys = kv_all.at[pl.ds(first * per, size * per), pl.ds(0, n_cp - 1)]
            pltpu.make_async_copy(keys, keys, k_recv.at[first]).wait()

    def reduce(k, h, dests=slice(None)):
        with jax.named_scope(f"reduce{k}{h}"):
            for u in units_of[k]:
                hop(u, h, dests)

    with jax.named_scope("fill"):
        for source in range(n_cp):
            take(source)
            end_sends(source)
            if source < 2:
                flow(source, 0, False)
            if source < LEAD:
                flow(source, 0, True)
        for source in range(2):
            for d in range(1, end):
                flow(source, d, False)
            if source == 1:
                flow(2, 0, False)
            if end > 1:
                flow(source, 1, True)
        for source in range(2):
            for d in range(2, end):
                flow(source, d, True)
        flow(LEAD, 0, True)
        far(2)
        ends(0)
    pltpu.make_async_copy(w, w, w_sem).wait()
    passed, reached = 2, 1

    def pass_on(fars, nears):
        nonlocal passed, reached
        while passed < min(fars, n_cp - 1):
            passed += 1
            far(passed)
        while reached < min(nears, n_cp - 1):
            reached += 1
            near(reached)

    parts = (slice(0, 1), slice(1, None))
    hops = [(k, h, p) for k in range(last) for h in range(1, end) for p in range(min(2, n_tp - 1 - h))]
    held = {}

    def run(k, h, *wanted):
        for p in wanted:
            if (k, h, p) in hops:
                hops.remove((k, h, p))
                reduce(k, h, parts[p])

    def weave(k):
        left = [(h, p) for e, h, p in hops if e == k]
        with jax.named_scope("weave"):
            for u in units_of[k]:
                for h, p in left:
                    hop(u, h, parts[p])
        for h, p in left:
            hops.remove((k, h, p))

    def projection(k):
        pass_on(0, firsts[k + 1] - 1)
        for group in groups[k]:
            for source in range(max(group[0], 1), group[0] + group[1]):
                ends(source)
            with jax.named_scope("keys"):
                project_keys(group)
        with jax.named_scope("queries"):
            project_queries(k)

    def attention(k):
        with jax.named_scope("attend"):
            held[k] = attend(k)

    def result(k):
        with jax.named_scope("output"):
            output(k, held.pop(k))

    def adjacents(*chosen):
        for k in chosen:
            adjacent(k)

    if last == 4:
        plan = [
            (projection, 0), (pass_on, 5, 3), (attention, 0), (pass_on, 6, 4),
            (result, 0), (adjacents, 0),
            (projection, 1), (pass_on, n_cp, 6), (attention, 1), (pass_on, n_cp, n_cp),
            (result, 1), (adjacents, 1), (run, 0, 1, 0, 1),
            (projection, 2), (attention, 2), (run, 1, 1, 0),
            (result, 2), (adjacents, 2), (run, 1, 1, 1), (run, 0, 2, 0),
            (projection, 3), (run, 1, 2, 0), (run, 2, 1, 0), (attention, 3),
            (result, 3), (adjacents, 3),
            (run, 2, 1, 1), (run, 2, 2, 0), (run, 3, 1, 0), (weave, 3),
        ]
    else:
        plan = []
        for k in range(last):
            plan += [(projection, k), (pass_on, n_cp, n_cp), (attention, k), (result, k), (adjacents, k)]
    pltpu.make_async_copy(wo, wo, o_sem).wait()
    for step, *given in plan:
        step(*given)
    for k, h, p in list(hops):
        reduce(k, h, parts[p])
    with jax.named_scope("finish"):
        for u in range(len(spans)):
            finish(u)

    with jax.named_scope("a2a"):
        for b in range(blocks):
            outgoing[b] = done[order[b]]
        for i in range(1, n_cp):
            final(i).start()
        out_ref[:, pl.ds(c, 1)] = outgoing[pl.ds(c * per, per)][:, None]
        others = landed.at[:, pl.ds(0, n_cp - 1)]
        pltpu.make_async_copy(others, others, a_recv).wait()
        for i in range(1, n_cp):
            source = lax.rem(c - i + n_cp, n_cp)
            out_ref[:, pl.ds(source, 1)] = landed[:, pl.ds(source, 1)]

    def drain(ref, sem):
        pltpu.make_async_copy(ref, ref, sem).wait()

    drain(landed.at[:, pl.ds(0, n_cp - 1)], s_send)
    drain(landed.at[:, pl.ds(0, n_cp - 1)], a_send)
    drain(kv_all.at[:, pl.ds(0, n_cp - 1)], k_send)
    for v in range(n_tp):
        @pl.when(z == v)
        def _():
            if v < end:
                drain(rows.at[pl.ds(0, v + 1)], r_send)
                drain(to_right.at[pl.ds(0, end - v)], pr_send)
            if v > 0:
                drain(rows.at[pl.ds(0, n_tp - v)], l_send)
                drain(to_left.at[pl.ds(0, v)], pl_send)


def fused_call(bounds, owner, hidden, wq, wk, wv, wo, inverse, n_cp, n_tp):
    rows, width = hidden.shape
    per = rows // BLOCK
    share = BLOCK // n_cp
    blocks = per * n_cp
    heads = wq.shape[1] // HEAD_WIDTH
    sizes = chunk_sizes(n_cp)
    pieces = hidden.reshape(per, n_cp, share, width)
    bf, f32, i32, dma = jnp.bfloat16, jnp.float32, jnp.int32, pltpu.SemaphoreType.DMA
    vmem = pl.BlockSpec(memory_space=pltpu.VMEM)
    hbm = pl.BlockSpec(memory_space=pltpu.HBM)
    smem = pl.BlockSpec(memory_space=pltpu.SMEM)
    slab = (n_tp, rows, width)
    kv_width = 2 * HEAD_WIDTH
    sums = dma((n_tp - 1, len(sizes) - 1 + sizes[-1] * per))
    flops = 2 * rows * (wq.shape[0] * (wq.shape[1] + kv_width) + wo.shape[0] * wo.shape[1])
    out = pl.pallas_call(
        functools.partial(fused_kernel, n_cp, n_tp, sizes, bounds.shape[0]),
        out_shape=jax.ShapeDtypeStruct((per, n_cp, share, width), bf),
        in_specs=[smem, hbm, hbm, hbm, hbm, hbm, vmem],
        out_specs=vmem,
        scratch_shapes=[
            pltpu.VMEM((per, n_cp, share, width), bf),
            pltpu.VMEM((n_tp, blocks, share, width), bf),
            pltpu.VMEM((wq.shape[0], wq.shape[1] + kv_width), bf),
            pltpu.VMEM((n_tp, wo.shape[0], width), bf),
            pltpu.VMEM((rows, HEAD_WIDTH), f32), pltpu.VMEM((rows, HEAD_WIDTH), f32),
            pltpu.VMEM((rows, HEAD_WIDTH), i32), pltpu.VMEM((rows, HEAD_WIDTH), i32),
            pltpu.VMEM((rows * heads, HEAD_WIDTH), bf),
            pltpu.VMEM((blocks, share, kv_width), bf),
            pltpu.VMEM((blocks, n_cp, share, kv_width), bf),
            pltpu.VMEM(slab, f32),
            pltpu.VMEM(slab, bf), pltpu.VMEM(slab, bf), pltpu.VMEM(slab, bf), pltpu.VMEM(slab, bf),
            pltpu.VMEM((blocks, share, width), bf),
            pltpu.VMEM((blocks, share, width), bf),
            pltpu.VMEM((per, n_cp, share, width), bf),
            pltpu.SMEM((blocks,), i32),
            dma, dma, dma, dma, dma, dma((n_cp,)), dma, dma, dma((n_tp, n_cp)),
            dma, dma((n_cp,)), dma, dma, sums, sums, dma, dma,
        ],
        compiler_params=pltpu.CompilerParams(
            collective_id=1, has_side_effects=True, vmem_limit_bytes=VMEM_LIMIT
        ),
        cost_estimate=pl.CostEstimate(flops=flops, bytes_accessed=20 << 20, transcendentals=0),
    )(jnp.concatenate([bounds, owner]), pieces, wq, wk, wv, wo, inverse)
    return out.reshape(rows, width)


def local_fused(
    hidden, query_weight, key_matrix, value_matrix, output_weight, document_bounds, block_owner
):
    n_cp, n_tp = lax.axis_size("cp"), lax.axis_size("tp")
    inverse = jnp.tile(rope_inverse(HEAD_WIDTH), 2)[None, :]
    return fused_call(
        document_bounds, block_owner, hidden, query_weight, key_matrix, value_matrix,
        output_weight, inverse, n_cp, n_tp,
    )


def local_plain(
    hidden, query_weight, key_matrix, value_matrix, output_weight, document_bounds, block_owner
):
    cp_index = lax.axis_index("cp")
    row_count = hidden.shape[0]
    per_device = row_count // BLOCK
    block_order = owner_order(block_owner, per_device)
    own_blocks = lax.dynamic_slice_in_dim(block_order, cp_index * per_device, per_device, 0)
    new_tokens = (
        own_blocks[:, None] * BLOCK + jnp.arange(BLOCK, dtype=jnp.int32)[None, :]
    ).reshape(-1)
    kv_heads = key_matrix.shape[1] // HEAD_WIDTH
    moved = relayout(hidden, block_order)
    query_raw, key_raw, value_raw = project(moved, query_weight, key_matrix, value_matrix)
    queries = rotate(query_raw, new_tokens, document_bounds, HEAD_WIDTH)
    key_rows = rotate(key_raw, new_tokens, document_bounds, HEAD_WIDTH)
    value_rows = value_raw.astype(jnp.bfloat16)
    heads_out = attend(
        queries, new_tokens, key_rows, value_rows, new_tokens, document_bounds, HEAD_WIDTH, kv_heads
    )
    return output_rows(heads_out, output_weight)


def solution(mesh):
    shares = BLOCK // mesh.shape["cp"]
    local = local_fused if shares % 16 == 0 else local_plain
    placed = (P("cp", "tp"), P(None, "tp"), P(None, "tp"), P(None, "tp"), P("tp", None), P(), P())
    return jax.shard_map(
        local, mesh=mesh, in_specs=placed, out_specs=P("cp", "tp"), check_vma=False
    )
```

```python
import functools
import math

import jax
import jax.numpy as jnp
from jax import lax
from jax.experimental import pallas as pl
from jax.experimental.pallas import tpu as pltpu
from jax.sharding import PartitionSpec as P

HEAD_WIDTH = 128
BLOCK = 128


rope_theta = 500000.0
rope_factor = 8.0
rope_context = 8192.0
masked_score = -1e30


def rope_inverse(head_size):
    halves = jnp.arange(head_size // 2, dtype=jnp.float32)
    inverse = 1.0 / rope_theta ** (2.0 * halves / head_size)
    wavelength = 2.0 * math.pi / inverse
    smooth = (rope_context / wavelength - 1.0) / 3.0
    blended = (1.0 - smooth) * inverse / rope_factor + smooth * inverse
    longer = jnp.where(wavelength > rope_context, inverse / rope_factor, blended)
    return jnp.where(wavelength < rope_context / 4.0, inverse, longer)


def document_of(tokens, bounds):
    inner_bounds = bounds[1:-1]
    return jnp.sum((tokens[:, None] >= inner_bounds[None, :]).astype(jnp.int32), axis=1)


def position_of(tokens, bounds):
    starts = bounds[:-1]
    document_start = jnp.max(
        jnp.where(starts[None, :] <= tokens[:, None], starts[None, :], 0), axis=1
    )
    return tokens - document_start


def rotate(raw_rows, tokens, bounds, head_size):
    row_count = raw_rows.shape[0]
    head_count = raw_rows.shape[1] // head_size
    angles = (
        position_of(tokens, bounds).astype(jnp.float32)[:, None] * rope_inverse(head_size)[None, :]
    )
    cosine = jnp.cos(angles)[:, None, :]
    sine_table = jnp.sin(angles)[:, None, :]
    heads_view = raw_rows.reshape(row_count, head_count, head_size)
    front_half = heads_view[:, :, : head_size // 2]
    back_half = heads_view[:, :, head_size // 2 :]
    turned = jnp.concatenate(
        [
            front_half * cosine - back_half * sine_table,
            back_half * cosine + front_half * sine_table,
        ],
        axis=2,
    )
    return turned.reshape(row_count, head_count * head_size).astype(jnp.bfloat16)


def owner_order(block_owner, per_device):
    block_count = block_owner.shape[0]
    blocks = jnp.arange(block_count, dtype=jnp.int32)
    same_owner = block_owner[:, None] == block_owner[None, :]
    earlier = blocks[None, :] < blocks[:, None]
    owner_rank = jnp.sum((same_owner & earlier).astype(jnp.int32), axis=1)
    target = block_owner * per_device + owner_rank
    return jnp.sum(jnp.where(target[None, :] == blocks[:, None], blocks[None, :], 0), axis=1)


def relayout(local_rows, block_order):
    cp_size = lax.axis_size("cp")
    row_count, row_width = local_rows.shape
    per_device = row_count // BLOCK
    portion = BLOCK // cp_size
    pieces = local_rows.reshape(per_device, cp_size, portion * row_width)
    spread = lax.all_to_all(pieces, "cp", split_axis=1, concat_axis=0, tiled=True)
    spread = spread.reshape(per_device * cp_size, portion * row_width)
    wanted = block_order.reshape(cp_size, per_device).T.reshape(-1)
    outgoing = jnp.take(spread, wanted, axis=0).reshape(per_device, cp_size, portion * row_width)
    arrived = lax.all_to_all(outgoing, "cp", split_axis=1, concat_axis=1, tiled=True)
    return arrived.reshape(row_count, row_width)


def project(local_rows, query_weight, key_matrix, value_matrix):
    weight_list = (query_weight, key_matrix, value_matrix)
    portion = lax.all_gather(local_rows, "tp", axis=1, tiled=True)
    return tuple(
        (jnp.dot(portion, weight, preferred_element_type=jnp.float32) for weight in weight_list)
    )


def attend(queries, query_tokens, key_rows, value_rows, key_tokens, bounds, head_size, kv_heads):
    row_count = queries.shape[0]
    query_group_width = queries.shape[1] // (kv_heads * head_size)
    grouped = queries.reshape(row_count, kv_heads, query_group_width, head_size).transpose(
        1, 2, 0, 3
    )
    grouped = grouped.reshape(kv_heads, query_group_width * row_count, head_size)
    query_documents = document_of(query_tokens, bounds)
    score_scale = 1.0 / math.sqrt(head_size)

    def update(flash_state, key_block, value_block, token_block):
        block_rows = key_block.shape[0]
        key_documents = document_of(token_block, bounds)
        allowed = (query_documents[:, None] == key_documents[None, :]) & (
            token_block[None, :] <= query_tokens[:, None]
        )
        running_max, running_sum, running_out = flash_state
        per_head_keys = key_block.reshape(block_rows, kv_heads, head_size).transpose(1, 0, 2)
        per_head_values = value_block.reshape(block_rows, kv_heads, head_size).transpose(1, 0, 2)
        scores = (
            jnp.einsum("khd,ksd->khs", grouped, per_head_keys, preferred_element_type=jnp.float32)
            * score_scale
        )
        wide_mask = jnp.tile(allowed, (query_group_width, 1))[None, :, :]
        scores = jnp.where(wide_mask, scores, masked_score)
        new_max = jnp.maximum(running_max, jnp.max(scores, axis=2))
        weights = jnp.where(wide_mask, jnp.exp(scores - new_max[:, :, None]), 0.0)
        factor = jnp.exp(running_max - new_max)
        new_sum = running_sum * factor + jnp.sum(weights, axis=2)
        new_out = running_out * factor[:, :, None] + jnp.einsum(
            "khs,ksd->khd",
            weights.astype(jnp.bfloat16),
            per_head_values,
            preferred_element_type=jnp.float32,
        )
        return (new_max, new_sum, new_out)

    initial = (
        jnp.full((kv_heads, query_group_width * row_count), masked_score, jnp.float32),
        jnp.zeros((kv_heads, query_group_width * row_count), jnp.float32),
        jnp.zeros((kv_heads, query_group_width * row_count, head_size), jnp.float32),
    )
    key_part = lax.all_gather(key_rows, "cp", axis=0, tiled=True)
    value_part = lax.all_gather(value_rows, "cp", axis=0, tiled=True)
    token_part = lax.all_gather(key_tokens, "cp", axis=0, tiled=True)
    part_rows = key_part.shape[0]
    block_rows = math.gcd(part_rows, 512)

    def one_block(block_index, inner_state):
        first_row = block_index * block_rows
        return update(
            inner_state,
            lax.dynamic_slice_in_dim(key_part, first_row, block_rows, 0),
            lax.dynamic_slice_in_dim(value_part, first_row, block_rows, 0),
            lax.dynamic_slice_in_dim(token_part, first_row, block_rows, 0),
        )

    final_max, final_sum, final_out = lax.fori_loop(0, part_rows // block_rows, one_block, initial)
    normalized = final_out / final_sum[:, :, None]
    merged = normalized.reshape(kv_heads, query_group_width, row_count, head_size).transpose(
        2, 0, 1, 3
    )
    return merged.reshape(row_count, kv_heads * query_group_width * head_size).astype(jnp.bfloat16)


def output_rows(heads_out, output_weight):
    head_terms = jnp.dot(heads_out, output_weight, preferred_element_type=jnp.float32)
    return lax.psum_scatter(head_terms.astype(jnp.bfloat16), "tp", scatter_dimension=1, tiled=True)


MESH = pl.DeviceIdType.MESH
VMEM_LIMIT = 53 << 20
PASS_ROWS = 128
LEAD = 3


def dot(a, b):
    return jnp.dot(a, b, preferred_element_type=jnp.float32)


def fill_rows(x):
    copies = max(PASS_ROWS // x.shape[0], 1)
    return jnp.concatenate([x] * copies, axis=0) if copies > 1 else x


def turn(raw, cosine, sine):
    half = raw.shape[1] // 2
    swapped = jnp.concatenate([raw[:, half:], raw[:, :half]], axis=1)
    return (raw * cosine + swapped * sine).astype(jnp.bfloat16)


def greet(n_cp, n_tp):
    c, z = lax.axis_index("cp"), lax.axis_index("tp")
    barrier = pltpu.get_barrier_semaphore()
    for t in range(1, n_cp):
        peer = lax.rem(c + t, n_cp)
        pl.semaphore_signal(barrier, inc=1, device_id={"cp": peer}, device_id_type=MESH)
    for t in range(1, n_tp):
        peer = lax.rem(z + t, n_tp)
        pl.semaphore_signal(barrier, inc=1, device_id={"tp": peer}, device_id_type=MESH)
    pl.semaphore_wait(barrier, n_cp + n_tp - 2)


def row_tokens(bounds, blocks, share, offset):
    shape = (blocks, share, HEAD_WIDTH)
    token = (
        lax.broadcasted_iota(jnp.int32, shape, 0) * BLOCK
        + lax.broadcasted_iota(jnp.int32, shape, 1) + offset
    )
    start = jnp.zeros_like(token)
    for i in range(len(bounds) - 1):
        start = jnp.where(token >= bounds[i], bounds[i], start)
    return token, start


def chunk_sizes(sources):
    if sources < 4 or sources % 2:
        return [1] * sources
    return [2] * (sources // 2)


def fused_kernel(
    n_cp, n_tp, sizes, bound_count,
    table, hidden, wq_hbm, wk_hbm, wv_hbm, wo_hbm, inverse,
    out_ref,
    mine, rows, w, wo, cosine, sine, tokens, starts, q_all, kv_own, kv_all,
    part, from_left, from_right, to_right, to_left, done, outgoing, landed, order,
    w_sem, o_sem, own_sem, m_sem, s_send, s_recv, r_send, l_send, z_recv, k_send, k_recv,
    pr_send, pl_send, pr_recv, pl_recv, a_send, a_recv,
):
    c, z = lax.axis_index("cp"), lax.axis_index("tp")
    bounds = [table[i] for i in range(bound_count)]
    owner = [table[bound_count + b] for b in range(table.shape[0] - bound_count)]
    per, share, width = hidden.shape[0], hidden.shape[2], hidden.shape[3]
    blocks = per * n_cp
    unit = per * share
    q_width = wq_hbm.shape[1]
    heads = q_width // HEAD_WIDTH
    end = n_tp - 1
    last = len(sizes)
    firsts = [sum(sizes[:k]) for k in range(last + 1)]
    spans = [(firsts[k] * unit, sizes[k] * unit) for k in range(last - 1)]
    spans += [(firsts[last - 1] * unit + b * share, share) for b in range(sizes[-1] * per)]
    units_of = [[k] for k in range(last - 1)] + [list(range(last - 1, len(spans)))]
    groups = [[(a, 1) for a in range(firsts[k], firsts[k + 1])] for k in range(last)]
    factor_of = math.log2(math.e) / math.sqrt(HEAD_WIDTH)
    weights = (
        pltpu.make_async_copy(wk_hbm, w.at[:, pl.ds(q_width, HEAD_WIDTH)], w_sem),
        pltpu.make_async_copy(wv_hbm, w.at[:, pl.ds(q_width + HEAD_WIDTH, HEAD_WIDTH)], w_sem),
        pltpu.make_async_copy(wq_hbm, w.at[:, pl.ds(0, q_width)], w_sem),
    )

    def out_weight(o):
        return pltpu.make_async_copy(
            wo_hbm.at[:, pl.ds(o * width, width)], wo.at[o], o_sem
        )

    own = pltpu.make_async_copy(hidden.at[:, c], rows.at[z, pl.ds(c * per, per)], own_sem)
    staged = pltpu.make_async_copy(hidden, mine, m_sem)
    staged.start()
    own.start()
    greet(n_cp, n_tp)
    staged.wait()

    def across(i):
        peer, bit = 0, 1
        while bit < n_cp:
            mine_bit = lax.rem(lax.div(c, bit), 2)
            peer += bit * (1 - mine_bit if i // bit % 2 else mine_bit)
            bit *= 2
        return peer

    peers = range(n_cp - 1, 0, -1)

    def spread(i):
        peer = across(i)
        return pltpu.make_async_remote_copy(
            src_ref=mine.at[:, peer], dst_ref=rows.at[z, pl.ds(c * per, per)],
            send_sem=s_send, recv_sem=s_recv.at[i],
            device_id={"cp": peer}, device_id_type=MESH,
        )

    def along(origin, source, step):
        piece = rows.at[origin, pl.ds(source * per, per)]
        sems = r_send if step > 0 else l_send
        return pltpu.make_async_remote_copy(
            src_ref=piece, dst_ref=piece,
            send_sem=sems, recv_sem=z_recv.at[origin, source],
            device_id={"tp": lax.rem(z + step + n_tp, n_tp)}, device_id_type=MESH,
        )

    def blocks_of(k):
        return pl.ds(firsts[k] * per, sizes[k] * per)

    def lines_of(k):
        return pl.ds(firsts[k] * unit, sizes[k] * unit)

    def keys_to(i, group):
        span = pl.ds(group[0] * per, group[1] * per)
        return pltpu.make_async_remote_copy(
            src_ref=kv_own.at[span], dst_ref=kv_all.at[span, c],
            send_sem=k_send, recv_sem=k_recv.at[group[0]],
            device_id={"cp": across(i)}, device_id_type=MESH,
        )

    def rightward(o, u):
        lines = pl.ds(*spans[u])
        return pltpu.make_async_remote_copy(
            src_ref=to_right.at[o, lines], dst_ref=from_left.at[o, lines],
            send_sem=pr_send, recv_sem=pr_recv.at[o - 1, u],
            device_id={"tp": lax.rem(z + 1, n_tp)}, device_id_type=MESH,
        )

    def leftward(o, u):
        lines = pl.ds(*spans[u])
        return pltpu.make_async_remote_copy(
            src_ref=to_left.at[o, lines], dst_ref=from_right.at[o, lines],
            send_sem=pl_send, recv_sem=pl_recv.at[o, u],
            device_id={"tp": lax.rem(z + n_tp - 1, n_tp)}, device_id_type=MESH,
        )

    def final(i):
        peer = across(i)
        return pltpu.make_async_remote_copy(
            src_ref=outgoing.at[pl.ds(peer * per, per)], dst_ref=landed.at[:, c],
            send_sem=a_send, recv_sem=a_recv,
            device_id={"cp": peer}, device_id_type=MESH,
        )

    for i in peers:
        spread(i).start()
    for copy in weights:
        copy.start()
    for o in range(n_tp):
        out_weight(o).start()

    token, start = row_tokens(bounds, blocks, share, c * share)
    tokens[...] = token.reshape(-1, HEAD_WIDTH)
    starts[...] = start.reshape(-1, HEAD_WIDTH)
    angle = (token - start).astype(jnp.float32).reshape(-1, HEAD_WIDTH) * inverse[...]
    cosine[...] = jnp.cos(angle)
    lane = lax.broadcasted_iota(jnp.int32, angle.shape, 1)
    sine[...] = jnp.where(lane < HEAD_WIDTH // 2, -1.0, 1.0) * jnp.sin(angle)
    slots = []
    for b in range(blocks):
        rank = jnp.int32(0)
        for e in range(b):
            rank += (owner[e] == owner[b]).astype(jnp.int32)
        slots.append(owner[b] * per + rank)
    for b in range(blocks):
        found = jnp.int32(0)
        for e in range(1, blocks):
            found = jnp.where(slots[e] == b, e, found)
        order[b] = found
    own.wait()

    inner = (z > 0) & (z < end)

    def take(source):
        @pl.when(source != c)
        def _():
            landing = rows.at[z, pl.ds(source * per, per)]
            pltpu.make_async_copy(landing, landing, s_recv.at[across(source)]).wait()

    def end_sends(source):
        @pl.when(z == 0)
        def _():
            along(z, source, 1).start()

        @pl.when(z == end)
        def _():
            along(z, source, -1).start()

    def end_waits(source):
        for d in range(1, n_tp):
            @pl.when(z == end)
            def _():
                along(z - d, source, 1).wait_recv()

            @pl.when(z == 0)
            def _():
                along(z + d, source, -1).wait_recv()

    def flow(source, d, near):
        if source >= n_cp:
            return
        rights = (z == end - 1) if near else (z < end - 1)
        lefts = (z == 1) if near else (z > 1)

        @pl.when(inner & rights & (z - d >= 0))
        def _():
            if d > 0:
                along(z - d, source, 1).wait_recv()
            along(z - d, source, 1).start()

        @pl.when(inner & lefts & (z + d < n_tp))
        def _():
            if d > 0:
                along(z + d, source, -1).wait_recv()
            along(z + d, source, -1).start()

    def far(source):
        with jax.named_scope("far"):
            for d in range(1, end):
                flow(source, d, False)
            flow(source + 1, 0, False)

    def near(source):
        with jax.named_scope("near"):
            for d in range(1, end):
                flow(source, d, True)
            if source >= LEAD:
                flow(source + 1, 0, True)

    def ends(source):
        with jax.named_scope("ends"):
            end_waits(source)

    def gathered(first, size):
        span = pl.ds(first * per, size * per)
        count = size * unit
        x = [rows[o, span].reshape(count, width) for o in range(n_tp)]
        lines = pl.ds(first * unit, count)
        return fill_rows(jnp.concatenate(x, axis=1)), cosine[lines, :], sine[lines, :]

    def project_keys(group):
        count = group[1] * unit
        span = pl.ds(group[0] * per, group[1] * per)
        x, cos_t, sin_t = gathered(*group)
        raw = dot(x, w[:, q_width:])[:count]
        key = turn(raw[:, :HEAD_WIDTH], cos_t, sin_t)
        value = raw[:, HEAD_WIDTH:].astype(jnp.bfloat16)
        tile = jnp.concatenate([key, value], axis=1)
        tile = tile.reshape(group[1] * per, share, 2 * HEAD_WIDTH)
        kv_own[span] = tile
        kv_all[span, pl.ds(c, 1)] = tile[:, None]
        for i in peers:
            keys_to(i, group).start()

    def project_queries(k):
        count = sizes[k] * unit
        x, cos_t, sin_t = gathered(firsts[k], sizes[k])
        raw_q = dot(x, w[:, :q_width])[:count]
        for h in range(heads):
            q_all[pl.ds(firsts[k] * unit * heads + h * count, count), :] = turn(
                raw_q[:, h * HEAD_WIDTH : (h + 1) * HEAD_WIDTH], cos_t, sin_t
            )

    def attend(k):
        count = sizes[k] * unit
        q = q_all[pl.ds(firsts[k] * unit * heads, heads * count), :]
        start = jnp.tile(starts[lines_of(k), :], (heads, 1))[:, :1]
        token = jnp.tile(tokens[lines_of(k), :], (heads, 1))[:, :1]

        def scored(source, size, diagonal):
            keys = size * per * BLOCK
            span = pl.ds(source * per, size * per)
            key = kv_all[span, :, :, :HEAD_WIDTH].reshape(keys, HEAD_WIDTH)
            value = kv_all[span, :, :, HEAD_WIDTH:].reshape(keys, HEAD_WIDTH)
            score = lax.dot_general(
                q, key, (((1,), (1,)), ((), ())), preferred_element_type=jnp.float32
            )
            index = source * (per * BLOCK) + lax.broadcasted_iota(jnp.int32, score.shape, 1)
            allowed = index >= start
            if diagonal:
                allowed = allowed & (index <= token)
            return jnp.where(allowed, score, masked_score), value

        def lane_sums(weight):
            partial = weight[:, :HEAD_WIDTH]
            for g in range(1, weight.shape[1] // HEAD_WIDTH):
                partial = partial + weight[:, g * HEAD_WIDTH : (g + 1) * HEAD_WIDTH]
            return partial

        def more(source, size, diagonal, carry):
            top, total, out = carry
            score, value = scored(source, size, diagonal)
            new_top = jnp.maximum(top, jnp.max(score, axis=1, keepdims=True))
            weight = jnp.exp2((score - new_top) * factor_of)
            factor = jnp.exp2((top - new_top) * factor_of)
            total = total * factor + lane_sums(weight)
            out = out * factor + dot(weight.astype(jnp.bfloat16), value)
            return new_top, total, out

        lengths = (heads * count, 1)
        carry = (
            jnp.full(lengths, masked_score, jnp.float32),
            jnp.zeros((heads * count, HEAD_WIDTH), jnp.float32),
            jnp.zeros((heads * count, HEAD_WIDTH), jnp.float32),
        )
        pairs = firsts[k] // 2
        if pairs > 0:
            carry = lax.fori_loop(0, pairs, lambda j, held: more(2 * j, 2, False, held), carry)
        if firsts[k] % 2:
            carry = more(firsts[k] - 1, 1, False, carry)
        with jax.named_scope("kvwait"):
            arrive(k)
        carry = more(firsts[k], sizes[k], True, carry)
        _, total, out = carry
        out = (out / jnp.sum(total, axis=1, keepdims=True)).astype(jnp.bfloat16)
        return jnp.concatenate([out[h * count : (h + 1) * count] for h in range(heads)], axis=1)

    def output(k, attended):
        high = z // (n_tp // 2)
        count = attended.shape[0]
        attended = fill_rows(attended)
        for turn_of in range(n_tp):
            o = (1 - high) * (end - turn_of) + high * turn_of
            product = dot(attended, wo[o])[:count]
            go_right = (z == 0) & (o > z)
            go_left = (z == end) & (o < z)

            @pl.when(go_right)
            def _():
                to_right[o, lines_of(k)] = product.astype(jnp.bfloat16)

            @pl.when(go_left)
            def _():
                to_left[o, lines_of(k)] = product.astype(jnp.bfloat16)

            @pl.when(go_right & (o > z + 1))
            def _():
                for u in units_of[k]:
                    rightward(o, u).start()

            @pl.when(go_left & (o < z - 1))
            def _():
                for u in units_of[k]:
                    leftward(o, u).start()

            @pl.when(jnp.logical_not(go_right | go_left))
            def _():
                part[o, lines_of(k)] = product

    def adjacent(k):
        for u in units_of[k]:
            @pl.when(z == 0)
            def _():
                rightward(1, u).start()

            @pl.when(z == end)
            def _():
                leftward(end - 1, u).start()

    def hop(u, h, dests):
        lines = pl.ds(*spans[u])

        @pl.when(z == h)
        def _():
            for o in list(range(end, h, -1))[dests]:
                rightward(o, u).wait_recv()
                total = part[o, lines] + from_left[o, lines].astype(jnp.float32)
                to_right[o, lines] = total.astype(jnp.bfloat16)
                rightward(o, u).start()

        @pl.when(z == end - h)
        def _():
            for o in list(range(end - h))[dests]:
                leftward(o, u).wait_recv()
                total = part[o, lines] + from_right[o, lines].astype(jnp.float32)
                to_left[o, lines] = total.astype(jnp.bfloat16)
                leftward(o, u).start()

    def finish(u):
        lines = pl.ds(*spans[u])

        @pl.when(z > 0)
        def _():
            rightward(z, u).wait_recv()
            part[z, lines] += from_left[z, lines].astype(jnp.float32)

        @pl.when(z < end)
        def _():
            leftward(z, u).wait_recv()
            part[z, lines] += from_right[z, lines].astype(jnp.float32)

        summed = part[z, lines].astype(jnp.bfloat16)
        taken = pl.ds(spans[u][0] // share, spans[u][1] // share)
        done[taken] = summed.reshape(spans[u][1] // share, share, width)

    def arrive(k):
        for first, size in groups[k]:
            keys = kv_all.at[pl.ds(first * per, size * per), pl.ds(0, n_cp - 1)]
            pltpu.make_async_copy(keys, keys, k_recv.at[first]).wait()

    def reduce(k, h, dests=slice(None)):
        with jax.named_scope(f"reduce{k}{h}"):
            for u in units_of[k]:
                hop(u, h, dests)

    with jax.named_scope("fill"):
        for source in range(n_cp):
            take(source)
            end_sends(source)
            if source < 2:
                flow(source, 0, False)
            if source < LEAD:
                flow(source, 0, True)
        for source in range(2):
            for d in range(1, end):
                flow(source, d, False)
            if source == 1:
                flow(2, 0, False)
            if end > 1:
                flow(source, 1, True)
        for source in range(2):
            for d in range(2, end):
                flow(source, d, True)
        flow(LEAD, 0, True)
        far(2)
        ends(0)
    pltpu.make_async_copy(w, w, w_sem).wait()
    passed, reached = 2, 1

    def pass_on(fars, nears):
        nonlocal passed, reached
        while passed < min(fars, n_cp - 1):
            passed += 1
            far(passed)
        while reached < min(nears, n_cp - 1):
            reached += 1
            near(reached)

    parts = (slice(0, 1), slice(1, None))
    hops = [(k, h, p) for k in range(last) for h in range(1, end) for p in range(min(2, n_tp - 1 - h))]
    held = {}

    def run(k, h, *wanted):
        for p in wanted:
            if (k, h, p) in hops:
                hops.remove((k, h, p))
                reduce(k, h, parts[p])

    def weave(k):
        left = [(h, p) for e, h, p in hops if e == k]
        with jax.named_scope("weave"):
            for u in units_of[k]:
                for h, p in left:
                    hop(u, h, parts[p])
        for h, p in left:
            hops.remove((k, h, p))

    def projection(k):
        pass_on(0, firsts[k + 1] - 1)
        for group in groups[k]:
            for source in range(max(group[0], 1), group[0] + group[1]):
                ends(source)
            with jax.named_scope("keys"):
                project_keys(group)
        with jax.named_scope("queries"):
            project_queries(k)

    def attention(k):
        with jax.named_scope("attend"):
            held[k] = attend(k)

    def result(k):
        with jax.named_scope("output"):
            output(k, held.pop(k))

    def adjacents(*chosen):
        for k in chosen:
            adjacent(k)

    if last == 4:
        plan = [
            (projection, 0), (pass_on, 5, 3), (attention, 0), (pass_on, 6, 4),
            (result, 0), (adjacents, 0),
            (projection, 1), (pass_on, n_cp, 6), (attention, 1), (pass_on, n_cp, n_cp),
            (result, 1), (adjacents, 1), (run, 0, 1, 0, 1),
            (projection, 2), (attention, 2), (run, 1, 1, 0),
            (result, 2), (adjacents, 2), (run, 1, 1, 1), (run, 0, 2, 0),
            (projection, 3), (run, 1, 2, 0), (run, 2, 1, 0), (attention, 3),
            (result, 3), (adjacents, 3),
            (run, 2, 1, 1), (run, 2, 2, 0), (run, 3, 1, 0), (weave, 3),
        ]
    else:
        plan = []
        for k in range(last):
            plan += [(projection, k), (pass_on, n_cp, n_cp), (attention, k), (result, k), (adjacents, k)]
    pltpu.make_async_copy(wo, wo, o_sem).wait()
    for step, *given in plan:
        step(*given)
    for k, h, p in list(hops):
        reduce(k, h, parts[p])
    with jax.named_scope("finish"):
        for u in range(len(spans)):
            finish(u)

    with jax.named_scope("a2a"):
        for b in range(blocks):
            outgoing[b] = done[order[b]]
        for i in peers:
            final(i).start()
        out_ref[:, pl.ds(c, 1)] = outgoing[pl.ds(c * per, per)][:, None]
        others = landed.at[:, pl.ds(0, n_cp - 1)]
        pltpu.make_async_copy(others, others, a_recv).wait()
        for i in range(1, n_cp):
            source = across(i)
            out_ref[:, pl.ds(source, 1)] = landed[:, pl.ds(source, 1)]

    def drain(ref, sem):
        pltpu.make_async_copy(ref, ref, sem).wait()

    drain(landed.at[:, pl.ds(0, n_cp - 1)], s_send)
    drain(landed.at[:, pl.ds(0, n_cp - 1)], a_send)
    drain(kv_all.at[:, pl.ds(0, n_cp - 1)], k_send)
    for v in range(n_tp):
        @pl.when(z == v)
        def _():
            if v < end:
                drain(rows.at[pl.ds(0, v + 1)], r_send)
                drain(to_right.at[pl.ds(0, end - v)], pr_send)
            if v > 0:
                drain(rows.at[pl.ds(0, n_tp - v)], l_send)
                drain(to_left.at[pl.ds(0, v)], pl_send)


def fused_call(bounds, owner, hidden, wq, wk, wv, wo, inverse, n_cp, n_tp):
    rows, width = hidden.shape
    per = rows // BLOCK
    share = BLOCK // n_cp
    blocks = per * n_cp
    heads = wq.shape[1] // HEAD_WIDTH
    sizes = chunk_sizes(n_cp)
    pieces = hidden.reshape(per, n_cp, share, width)
    bf, f32, i32, dma = jnp.bfloat16, jnp.float32, jnp.int32, pltpu.SemaphoreType.DMA
    vmem = pl.BlockSpec(memory_space=pltpu.VMEM)
    hbm = pl.BlockSpec(memory_space=pltpu.HBM)
    smem = pl.BlockSpec(memory_space=pltpu.SMEM)
    slab = (n_tp, rows, width)
    kv_width = 2 * HEAD_WIDTH
    sums = dma((n_tp - 1, len(sizes) - 1 + sizes[-1] * per))
    flops = 2 * rows * (wq.shape[0] * (wq.shape[1] + kv_width) + wo.shape[0] * wo.shape[1])
    out = pl.pallas_call(
        functools.partial(fused_kernel, n_cp, n_tp, sizes, bounds.shape[0]),
        out_shape=jax.ShapeDtypeStruct((per, n_cp, share, width), bf),
        in_specs=[smem, hbm, hbm, hbm, hbm, hbm, vmem],
        out_specs=vmem,
        scratch_shapes=[
            pltpu.VMEM((per, n_cp, share, width), bf),
            pltpu.VMEM((n_tp, blocks, share, width), bf),
            pltpu.VMEM((wq.shape[0], wq.shape[1] + kv_width), bf),
            pltpu.VMEM((n_tp, wo.shape[0], width), bf),
            pltpu.VMEM((rows, HEAD_WIDTH), f32), pltpu.VMEM((rows, HEAD_WIDTH), f32),
            pltpu.VMEM((rows, HEAD_WIDTH), i32), pltpu.VMEM((rows, HEAD_WIDTH), i32),
            pltpu.VMEM((rows * heads, HEAD_WIDTH), bf),
            pltpu.VMEM((blocks, share, kv_width), bf),
            pltpu.VMEM((blocks, n_cp, share, kv_width), bf),
            pltpu.VMEM(slab, f32),
            pltpu.VMEM(slab, bf), pltpu.VMEM(slab, bf), pltpu.VMEM(slab, bf), pltpu.VMEM(slab, bf),
            pltpu.VMEM((blocks, share, width), bf),
            pltpu.VMEM((blocks, share, width), bf),
            pltpu.VMEM((per, n_cp, share, width), bf),
            pltpu.SMEM((blocks,), i32),
            dma, dma, dma, dma, dma, dma((n_cp,)), dma, dma, dma((n_tp, n_cp)),
            dma, dma((n_cp,)), dma, dma, sums, sums, dma, dma,
        ],
        compiler_params=pltpu.CompilerParams(
            collective_id=1, has_side_effects=True, vmem_limit_bytes=VMEM_LIMIT
        ),
        cost_estimate=pl.CostEstimate(flops=flops, bytes_accessed=20 << 20, transcendentals=0),
    )(jnp.concatenate([bounds, owner]), pieces, wq, wk, wv, wo, inverse)
    return out.reshape(rows, width)


def local_fused(
    hidden, query_weight, key_matrix, value_matrix, output_weight, document_bounds, block_owner
):
    n_cp, n_tp = lax.axis_size("cp"), lax.axis_size("tp")
    inverse = jnp.tile(rope_inverse(HEAD_WIDTH), 2)[None, :]
    return fused_call(
        document_bounds, block_owner, hidden, query_weight, key_matrix, value_matrix,
        output_weight, inverse, n_cp, n_tp,
    )


def local_plain(
    hidden, query_weight, key_matrix, value_matrix, output_weight, document_bounds, block_owner
):
    cp_index = lax.axis_index("cp")
    row_count = hidden.shape[0]
    per_device = row_count // BLOCK
    block_order = owner_order(block_owner, per_device)
    own_blocks = lax.dynamic_slice_in_dim(block_order, cp_index * per_device, per_device, 0)
    new_tokens = (
        own_blocks[:, None] * BLOCK + jnp.arange(BLOCK, dtype=jnp.int32)[None, :]
    ).reshape(-1)
    kv_heads = key_matrix.shape[1] // HEAD_WIDTH
    moved = relayout(hidden, block_order)
    query_raw, key_raw, value_raw = project(moved, query_weight, key_matrix, value_matrix)
    queries = rotate(query_raw, new_tokens, document_bounds, HEAD_WIDTH)
    key_rows = rotate(key_raw, new_tokens, document_bounds, HEAD_WIDTH)
    value_rows = value_raw.astype(jnp.bfloat16)
    heads_out = attend(
        queries, new_tokens, key_rows, value_rows, new_tokens, document_bounds, HEAD_WIDTH, kv_heads
    )
    return output_rows(heads_out, output_weight)


def solution(mesh):
    shares = BLOCK // mesh.shape["cp"]
    local = local_fused if shares % 16 == 0 else local_plain
    placed = (P("cp", "tp"), P(None, "tp"), P(None, "tp"), P(None, "tp"), P("tp", None), P(), P())
    return jax.shard_map(
        local, mesh=mesh, in_specs=placed, out_specs=P("cp", "tp"), check_vma=False
    )
```
